32 devices in a mesh: group: 8 (over z, core), member: 4 (over y, x).
Axes of the slice: x: 2, y: 2, z: 4, core: 2. Of those that a mesh axis runs over, the one named last changes fastest.
Arguments:
- rhs: bfloat16 [8, 4, 768, 128], P('group', 'member'), may hold values from -6 to 6
- leaf_pivot_inverse: bfloat16 [8, 4, 768, 768], P('group', 'member'), may hold values from -1.5 to 1.5, as said below
- leaf_border_block: bfloat16 [8, 4, 512, 768], P('group', 'member'), may hold values from -0.21875 to 0.21875
- leaf_map: int32 [8, 4, 4], P('group'), may hold values from 0 to 47, as said below
- mid_inverse: bfloat16 [8, 2048, 2048], P('group', 'member'), may hold values from -1.5 to 1.5, as said below
- mid_border: bfloat16 [8, 4096, 2048], P('group', None, 'member'), may hold values from -0.125 to 0.125
- root_map: int32 [8, 4, 8], P('group', 'member'), may hold values from 0 to 15, as said below
- root_inverse: bfloat16 [8192, 8192], P('group', 'member'), may hold values from -0.5 to 0.5, as said below
Outputs:
- leaf_solution: bfloat16 [8, 4, 768, 128], P('group', 'member')
- mid_solution: bfloat16 [8, 2048, 128], P('group', 'member')
- root_solution: bfloat16 [4, 2048, 128], P('member', 'group')
The draws below stay inside these ranges and needn't reach their ends.
Inputs may be any that keep to these rules, and one draw needn't show every extreme that they name: `leaf_map`: for each (g, m) the 4 entries are distinct; a value k below 16 names pivot block k of the mid-level front, a larger one border block k - 16. `root_map`: for each (g, m) the entries are distinct. `leaf_pivot_inverse`: each [768, 768] matrix is lower triangular with a positive diagonal, as the inverse of a Cholesky factor is: every entry above the diagonal is zero. `mid_inverse`: each [2048, 2048] matrix is lower triangular with a positive diagonal, as the inverse of a Cholesky factor is: every entry above the diagonal is zero. `root_inverse`: lower triangular with a positive diagonal, as the inverse of a Cholesky factor is: every entry above the diagonal is zero.
All inputs are finite; a program needn't handle non-finite values.
Results may differ from the reference program's by a relative error of at most 0.028.
Values may be sent and summed in bfloat16 or wider, within the bound.
No kernel may reach another device: no remote copies, remote signals or barrier semaphores. Data moves between devices by JAX's collectives and lax.ppermute only.
A program may use at most 64 MiB of HBM per device.

```python
import math
import jax
import jax.numpy as jnp
from jax import lax

P0 = 768
B0 = 512
P1 = 2048
B1 = 4096
ROOT = 8192
BLOCK = 128
R = 128
GROUPS = 8
MEMBERS = 4


def lower_factor(key, amount, size_order, scale_level):
    row_ids = lax.broadcasted_iota(jnp.int32, (size_order, size_order), 0)
    col_ids = lax.broadcasted_iota(jnp.int32, (size_order, size_order), 1)

    def one_factor(front_count):
        subkey = jax.random.fold_in(key, front_count)
        key_lower, key_diagonal = jax.random.split(subkey)
        values = jnp.clip(jax.random.normal(key_lower, (size_order, size_order), jnp.float32), -4.0, 4.0)
        diagonal = jax.random.uniform(key_diagonal, (size_order,), jnp.float32, 0.6, 1.4)
        lower_part = jnp.where(row_ids > col_ids, values * (0.9 / math.sqrt(size_order)), 0.0)
        return scale_level * (lower_part + jnp.where(row_ids == col_ids, diagonal[:, None], 0.0))
    return lax.map(one_factor, jnp.arange(amount, dtype=jnp.int32))


def distinct_picks(key, amount, pool_size, picked_count):
    scores = jax.random.randint(key, (amount, pool_size), 0, 1 << 20, jnp.int32) * pool_size
    scores = scores + lax.broadcasted_iota(jnp.int32, (amount, pool_size), 1)
    ranking = jnp.argsort(scores, axis=1, stable=True)
    return ranking[:, :picked_count].astype(jnp.int32)


def draw_leaf_pivot_inverse(key, part):
    factor = lower_factor(jax.random.fold_in(key, 1), GROUPS * MEMBERS, P0, 1.0)
    return factor.reshape(GROUPS, MEMBERS, P0, P0).astype(jnp.bfloat16)


def draw_mid_inverse(key, part):
    factor = lower_factor(jax.random.fold_in(key, 2), GROUPS, P1, 0.7)
    return factor.astype(jnp.bfloat16)


def draw_root_inverse(key, part):
    factor = lower_factor(jax.random.fold_in(key, 3), 1, ROOT, 0.25)
    return factor.reshape(ROOT, ROOT).astype(jnp.bfloat16)


def draw_leaf_map(key, part):
    picks = distinct_picks(jax.random.fold_in(key, 11), GROUPS * MEMBERS, P1 // BLOCK + B1 // BLOCK, B0 // BLOCK)
    return picks.reshape(GROUPS, MEMBERS, B0 // BLOCK)


def draw_root_map(key, part):
    picks = distinct_picks(jax.random.fold_in(key, 12), GROUPS * MEMBERS, ROOT // (BLOCK * MEMBERS), B1 // (BLOCK * MEMBERS))
    return picks.reshape(GROUPS, MEMBERS, B1 // (BLOCK * MEMBERS))


def level_of(rng, extent, pieces, low, high):
    def one(axis_at, shards_of):
        heights = jax.random.uniform(jax.random.fold_in(jax.random.fold_in(rng, 6), axis_at), (shards_of,), jnp.float32, low / len(pieces), high / len(pieces))
        return jnp.repeat(jnp.exp(heights), extent[axis_at] // shards_of).reshape((-1,) + (1,) * (len(extent) - axis_at - 1))

    factor_of = one(*pieces[0])
    for cut in pieces[1:]:
        factor_of = factor_of * one(*cut)
    return factor_of


def noise(rng, extent, deviation, bound, pieces=(), kind=jnp.bfloat16):
    gain = level_of(rng, extent, pieces, -0.22, 0.18) if pieces else 1.0
    drawn = jax.random.normal(rng, extent, jnp.float32) * deviation * gain
    return jnp.minimum(jnp.maximum(drawn, -bound), bound).astype(kind)


def setup_inputs(seed: int = 0) -> dict:
    key_of = jax.random.split(jax.random.key(seed), 9)
    return {
        "rhs": noise(key_of[0], (GROUPS, MEMBERS, P0, R), 1.0, 6.0, ((0, 8), (1, 4))),
        "leaf_pivot_inverse": draw_leaf_pivot_inverse(jax.random.fold_in(key_of[8], 71), 0),
        "leaf_border_block": noise(key_of[2], (GROUPS, MEMBERS, B0, P0), P0 ** -0.5, 0.21875, ((0, 8), (1, 4))),
        "leaf_map": draw_leaf_map(jax.random.fold_in(key_of[8], 71), 0),
        "mid_inverse": draw_mid_inverse(jax.random.fold_in(key_of[8], 71), 0),
        "mid_border": noise(key_of[5], (GROUPS, B1, P1), P1 ** -0.5, 0.125, ((0, 8), (2, 4))),
        "root_map": draw_root_map(jax.random.fold_in(key_of[8], 71), 0),
        "root_inverse": draw_root_inverse(jax.random.fold_in(key_of[8], 71), 0),
    }


def place_blocks(block_ids, targets, source_terms):
    selection_mask = (block_ids[:, None] == targets[None, :]).astype(jnp.float32)
    return jnp.einsum("ng,gcy->ncy", selection_mask, source_terms.astype(jnp.float32), precision=lax.Precision.HIGHEST)


def reference(rhs, leaf_pivot_inverse, leaf_border_block, leaf_map, mid_inverse, mid_border, root_map, root_inverse):
    groups = rhs.shape[0]
    members = rhs.shape[1]
    columns = rhs.shape[3]
    pivot_blocks = P1 // BLOCK
    front_blocks = pivot_blocks + B1 // BLOCK
    leaf_blocks = B0 // BLOCK
    per_member = B1 // (BLOCK * members)
    root_per = ROOT // (BLOCK * members)
    all_blocks = jnp.arange(front_blocks, dtype=jnp.int32)

    def forward_group(front_count):
        leaf_cholesky_factor = leaf_pivot_inverse[front_count].astype(jnp.float32)
        leaf_forward_solve = jnp.einsum("luc,lcd->lud", leaf_cholesky_factor, rhs[front_count].astype(jnp.float32)).astype(jnp.bfloat16)
        leaf_output = (-jnp.einsum("luc,lcd->lud", leaf_border_block[front_count].astype(jnp.float32), leaf_forward_solve.astype(jnp.float32))).astype(jnp.bfloat16)
        targets = leaf_map[front_count].reshape(members * leaf_blocks)
        front = place_blocks(all_blocks, targets, leaf_output.reshape(members * leaf_blocks, BLOCK, columns))
        front = front.reshape(front_blocks * BLOCK, columns)
        mid_rhs = front[:P1].astype(jnp.bfloat16)
        mid_forward = jnp.dot(mid_inverse[front_count], mid_rhs, preferred_element_type=jnp.float32).astype(jnp.bfloat16)
        mid_update = front[P1:] - jnp.dot(mid_border[front_count], mid_forward, preferred_element_type=jnp.float32)
        return leaf_forward_solve, mid_forward, mid_update

    leaf_forward_solve, mid_forward, mid_update = lax.map(forward_group, jnp.arange(groups, dtype=jnp.int32))
    chooser = (root_map[..., None] == jnp.arange(root_per, dtype=jnp.int32)).astype(jnp.float32)
    border_blocks = mid_update.reshape(groups, members, per_member, BLOCK * columns)
    root_rhs = jnp.einsum("gmiq,gmix->mqx", chooser, border_blocks, precision=lax.Precision.HIGHEST)
    root_rhs = root_rhs.reshape(ROOT, columns).astype(jnp.bfloat16)
    root_forward = jnp.dot(root_inverse, root_rhs, preferred_element_type=jnp.float32).astype(jnp.bfloat16)
    root_values = jnp.dot(root_inverse.T, root_forward, preferred_element_type=jnp.float32).astype(jnp.bfloat16)
    root_blocks = root_values.reshape(members, root_per, BLOCK * columns).astype(jnp.float32)
    border_values = jnp.einsum("gmiq,mqx->gmix", chooser, root_blocks, precision=lax.Precision.HIGHEST)
    border_values = border_values.astype(jnp.bfloat16).reshape(groups, B1, columns)

    def backward_group(front_count):
        border_here = border_values[front_count]
        mid_back = (mid_forward[front_count].astype(jnp.float32) - jnp.dot(mid_border[front_count].T, border_here, preferred_element_type=jnp.float32)).astype(jnp.bfloat16)
        inverse_row_set = mid_inverse[front_count].reshape(members, P1 // members, P1).astype(jnp.float32)
        backward_row_set = mid_back.reshape(members, P1 // members, columns).astype(jnp.float32)
        partial_value_rows = jnp.einsum("gxa,gxu->gau", inverse_row_set, backward_row_set).astype(jnp.bfloat16)
        mid_values = jnp.sum(partial_value_rows.astype(jnp.float32), axis=0).astype(jnp.bfloat16)
        front_values = jnp.concatenate([mid_values, border_here], axis=0).reshape(front_blocks, BLOCK, columns)
        targets = leaf_map[front_count].reshape(members * leaf_blocks)
        selected_items = place_blocks(targets, all_blocks, front_values).astype(jnp.bfloat16).reshape(members, B0, columns)
        leaf_backward_solve = (leaf_forward_solve[front_count].astype(jnp.float32) - jnp.einsum("aun,aue->ane", leaf_border_block[front_count].astype(jnp.float32), selected_items.astype(jnp.float32))).astype(jnp.bfloat16)
        leaf_value_rows = jnp.einsum("aun,aue->ane", leaf_pivot_inverse[front_count].astype(jnp.float32), leaf_backward_solve.astype(jnp.float32)).astype(jnp.bfloat16)
        return leaf_value_rows, mid_values

    leaf_solution, mid_solution = lax.map(backward_group, jnp.arange(groups, dtype=jnp.int32))
    return leaf_solution, mid_solution, root_values.reshape(members, ROOT // members, columns)
```

```python
import jax
import jax.numpy as jnp
from jax import lax
from jax.sharding import PartitionSpec as P

BLOCK = 128


def is_power_of_two(size):
    return size & (size - 1) == 0


def partner(index, step, size):
    return index ^ step if is_power_of_two(size) else (index + step) % size


def source(index, step, size):
    return index ^ step if is_power_of_two(size) else (index - step) % size


def exchange(values, axis, step, size):
    return lax.ppermute(values, axis, [(i, partner(i, step, size)) for i in range(size)])


def assemble(block_ids, targets, source_terms):
    selection_mask = (block_ids[:, None] == targets[None, :]).astype(jnp.bfloat16)
    return jnp.einsum(
        "ng,gcy->ncy", selection_mask, source_terms, preferred_element_type=jnp.float32
    )


def transposed(matrix, values):
    return lax.dot_general(
        matrix, values, (((0,), (0,)), ((), ())), preferred_element_type=jnp.float32
    )


def bf16_sum(values, other):
    return (values.astype(jnp.float32) + other.astype(jnp.float32)).astype(jnp.bfloat16)


def doubling(values, axis, steps, size):
    rows = values.shape[0] // 2
    low, high = values[:rows], values[rows:]
    for first, second in zip(steps, reversed(steps)):
        other_low = exchange(low, axis, first, size)
        other_high = exchange(high, axis, second, size)
        low, high = bf16_sum(low, other_low), bf16_sum(high, other_high)
    return jnp.concatenate([low, high], axis=0)


def member_sum(values, size):
    if not is_power_of_two(size):
        return lax.psum(values, "member")
    return doubling(values, "member", [1 << i for i in range(size.bit_length() - 1)], size)


def group_sum(values, size):
    if not is_power_of_two(size) or size < 2:
        return lax.psum(values, "group")
    core = lax.axis_index("group") & 1
    rows = values.shape[0] // 2
    mine = lax.dynamic_slice_in_dim(values, core * rows, rows, 0)
    other = lax.dynamic_slice_in_dim(values, (1 - core) * rows, rows, 0)
    mine = bf16_sum(mine, exchange(other, "group", 1, size))
    steps = [2 * ((2 << i) - 1) for i in range(size.bit_length() - 2)]
    mine = doubling(mine, "group", steps, size)
    other = exchange(mine, "group", 1, size)
    first = core == 0
    return jnp.concatenate([jnp.where(first, mine, other), jnp.where(first, other, mine)], axis=0)


def make_on_device(groups, members):
    steps = range(1, members)

    def on_device(
        rhs,
        leaf_pivot_inverse,
        leaf_border_block,
        leaf_map,
        mid_inverse,
        mid_border,
        root_map,
        root_inverse,
    ):
        member = lax.axis_index("member")
        leaf_source = rhs[0, 0]
        leaf_factor = leaf_pivot_inverse[0, 0]
        leaf_edge = leaf_border_block[0, 0]
        columns = leaf_source.shape[1]
        leaf_blocks = leaf_edge.shape[0] // BLOCK
        own_pivots = mid_inverse.shape[1]
        pivots = mid_inverse.shape[2]
        border_rows = mid_border.shape[1]
        pivot_blocks = pivots // BLOCK
        own_border = border_rows // members
        per_member = own_border // BLOCK
        group_maps = leaf_map[0]
        mid_factor = mid_inverse[0]
        mid_edge = mid_border[0]
        pivot_ids = jnp.arange(pivot_blocks, dtype=jnp.int32)

        def part(values, owner, rows):
            return lax.dynamic_slice_in_dim(values, owner * rows, rows, 0)

        leaf_forward = jnp.dot(leaf_factor, leaf_source, preferred_element_type=jnp.float32).astype(
            jnp.bfloat16
        )
        leaf_out = (-jnp.dot(leaf_edge, leaf_forward, preferred_element_type=jnp.float32)).astype(
            jnp.bfloat16
        )
        arrived = [leaf_out] + [exchange(leaf_out, "member", k, members) for k in steps]
        terms = jnp.concatenate(arrived, axis=0).reshape(members * leaf_blocks, BLOCK, columns)
        senders = jnp.stack([member] + [source(member, k, members) for k in steps])
        targets = group_maps[senders].reshape(members * leaf_blocks)
        mid_rhs = assemble(pivot_ids, targets, terms).reshape(pivots, columns).astype(jnp.bfloat16)
        border_ids = pivot_blocks + member * per_member + jnp.arange(per_member, dtype=jnp.int32)
        leaf_part = assemble(border_ids, targets, terms).reshape(own_border, columns)
        mid_forward = jnp.dot(mid_factor, mid_rhs, preferred_element_type=jnp.float32).astype(
            jnp.bfloat16
        )
        update = -jnp.dot(mid_edge, mid_forward, preferred_element_type=jnp.float32)
        sent = update.astype(jnp.bfloat16)
        arrived = [
            exchange(part(sent, partner(member, k, members), own_border), "member", k, members)
            for k in steps
        ]
        mid_update = part(update, member, own_border) + leaf_part
        for term in arrived:
            mid_update = mid_update + term.astype(jnp.float32)
        share_rows = root_inverse.shape[1]
        root_per = share_rows // BLOCK
        own_map = root_map[0, 0]
        chooser = own_map[:, None] == jnp.arange(root_per, dtype=jnp.int32)[None, :]
        chooser = chooser.astype(jnp.bfloat16)
        root_term = jnp.einsum(
            "iq,ix->qx",
            chooser,
            mid_update.astype(jnp.bfloat16).reshape(per_member, BLOCK * columns),
            preferred_element_type=jnp.float32,
        )
        root_rhs = group_sum(root_term.astype(jnp.bfloat16).reshape(share_rows, columns), groups)
        root_part = jnp.dot(root_inverse, root_rhs, preferred_element_type=jnp.float32)
        root_forward = member_sum(root_part.astype(jnp.bfloat16), members)
        back_part = transposed(root_inverse, root_forward)
        root_values = group_sum(back_part.astype(jnp.bfloat16), groups)
        rows_out = share_rows // groups
        root_out = part(root_values, lax.axis_index("group"), rows_out)[None]
        own_values = (
            jnp.einsum(
                "iq,qx->ix",
                chooser,
                root_values.reshape(root_per, BLOCK * columns),
                preferred_element_type=jnp.float32,
            )
            .astype(jnp.bfloat16)
            .reshape(own_border, columns)
        )
        border_values = jnp.zeros((border_rows, columns), jnp.bfloat16)
        border_values = lax.dynamic_update_slice_in_dim(
            border_values, own_values, member * own_border, 0
        )
        for k in steps:
            border_values = lax.dynamic_update_slice_in_dim(
                border_values,
                exchange(own_values, "member", k, members),
                source(member, k, members) * own_border,
                0,
            )
        mid_back = (mid_forward.astype(jnp.float32) - transposed(mid_edge, border_values)).astype(
            jnp.bfloat16
        )
        mid_part = transposed(mid_factor, mid_back).astype(jnp.bfloat16)
        part_blocks = mid_part.reshape(pivot_blocks, BLOCK, columns)

        def wanted(owner):
            asked = lax.dynamic_index_in_dim(group_maps, owner, 0, keepdims=False)
            return assemble(asked, pivot_ids, part_blocks)

        picked = wanted(member)
        for k in steps:
            blocks = wanted(partner(member, k, members)).astype(jnp.bfloat16)
            picked = picked + exchange(blocks, "member", k, members).astype(jnp.float32)
        own_targets = lax.dynamic_index_in_dim(group_maps, member, 0, keepdims=False)
        border_ids = pivot_blocks + jnp.arange(border_rows // BLOCK, dtype=jnp.int32)
        picked = picked + assemble(
            own_targets, border_ids, border_values.reshape(border_rows // BLOCK, BLOCK, columns)
        )
        picked = picked.astype(jnp.bfloat16).reshape(leaf_edge.shape[0], columns)
        mid_out = part(mid_part, member, own_pivots).astype(jnp.float32)
        for k in steps:
            rows = part(mid_part, partner(member, k, members), own_pivots)
            mid_out = mid_out + exchange(rows, "member", k, members).astype(jnp.float32)
        mid_out = mid_out.astype(jnp.bfloat16)[None]
        leaf_back = (leaf_forward.astype(jnp.float32) - transposed(leaf_edge, picked)).astype(
            jnp.bfloat16
        )
        leaf_values = transposed(leaf_factor, leaf_back).astype(jnp.bfloat16)
        return leaf_values[None, None], mid_out, root_out

    return on_device


def solution(mesh):
    in_specs = (
        P("group", "member", None, None),
        P("group", "member", None, None),
        P("group", "member", None, None),
        P("group", None, None),
        P("group", "member", None),
        P("group", None, "member"),
        P("group", "member", None),
        P("group", "member"),
    )
    out_specs = (
        P("group", "member", None, None),
        P("group", "member", None),
        P("member", "group", None),
    )
    on_device = make_on_device(mesh.shape["group"], mesh.shape["member"])
    return jax.shard_map(
        on_device, mesh=mesh, in_specs=in_specs, out_specs=out_specs, check_vma=False
    )
```

```python
import functools

import jax
import jax.numpy as jnp
from jax import lax
from jax.experimental import pallas as pl
from jax.experimental.pallas import tpu as pltpu
from jax.sharding import PartitionSpec as P

BLOCK = 128
VMEM_LIMIT = 20 * 1024 * 1024
F32 = jnp.float32
BF16 = jnp.bfloat16


def is_power_of_two(size):
    return size & (size - 1) == 0


def partner(index, step, size):
    return index ^ step if is_power_of_two(size) else (index + step) % size


def source(index, step, size):
    return index ^ step if is_power_of_two(size) else (index - step) % size


def exchange(values, axis, step, size):
    return lax.ppermute(values, axis, [(i, partner(i, step, size)) for i in range(size)])


def times_transpose(values, matrix):
    return lax.dot_general(values, matrix, (((1,), (1,)), ((), ())), preferred_element_type=F32)


def times(values, matrix):
    return jnp.dot(values, matrix, preferred_element_type=F32)


def traced_source(index, step, size):
    if is_power_of_two(size):
        return lax.bitwise_xor(index, jnp.int32(step))
    return lax.rem(index - step + size, jnp.int32(size))


def traced_partner(index, step, size):
    if is_power_of_two(size):
        return lax.bitwise_xor(index, jnp.int32(step))
    return lax.rem(index + step, jnp.int32(size))


def at_block(index):
    return pl.ds(pl.multiple_of(index * BLOCK, BLOCK), BLOCK)


def at_part(index, size):
    return pl.ds(pl.multiple_of(index * size, BLOCK), size)


def static_block(index):
    return pl.ds(index * BLOCK, BLOCK)


def leaf_forward_kernel(rhs_ref, factor_ref, edge_ref, forward_ref, out_ref):
    forward = times_transpose(rhs_ref[0, 0].T, factor_ref[0, 0]).astype(BF16)
    forward_ref[...] = forward
    out_ref[...] = (-times_transpose(forward, edge_ref[0, 0])).astype(BF16)


def mid_forward_kernel(members, *refs):
    map_ref, inverse_ref, border_ref = refs[:3]
    terms = refs[3 : 3 + members]
    forward_ref = refs[3 + members]
    sent = refs[4 + members : 3 + 2 * members]
    front = refs[-1]
    member = lax.axis_index("member")
    pivot_blocks = front.shape[1] // BLOCK
    front[...] = jnp.zeros_like(front)
    for k, term in enumerate(terms):
        owner = traced_source(member, k, members)
        for j in range(term.shape[1] // BLOCK):
            target = map_ref[0, owner, j]

            @pl.when(target < pivot_blocks)
            def _():
                front[:, at_block(target)] += term[:, static_block(j)].astype(F32)

    forward = times_transpose(front[...].astype(BF16), inverse_ref[0]).astype(BF16)
    forward_ref[...] = forward
    rows = sent[0].shape[1]
    for k, ref in enumerate(sent, start=1):
        owner = traced_partner(member, k, members)
        piece = border_ref[0, pl.ds(pl.multiple_of(owner * rows, BLOCK), rows), :]
        ref[...] = (-times_transpose(forward, piece)).astype(BF16)


def own_update_kernel(members, pivot_blocks, *refs):
    map_ref, border_ref, forward_ref = refs[:3]
    terms = refs[3 : 3 + members]
    update_ref = refs[-1]
    member = lax.axis_index("member")
    rows = update_ref.shape[1]
    piece = border_ref[0, pl.ds(pl.multiple_of(member * rows, BLOCK), rows), :]
    update_ref[...] = -times_transpose(forward_ref[...], piece)
    first = pivot_blocks + member * (rows // BLOCK)
    for k, term in enumerate(terms):
        owner = traced_source(member, k, members)
        for j in range(term.shape[1] // BLOCK):
            target = map_ref[0, owner, j] - first

            @pl.when((target >= 0) & (target < rows // BLOCK))
            def _():
                update_ref[:, at_block(target)] += term[:, static_block(j)].astype(F32)


def pieces_of(core, chips, groups, half):
    if chips == 1:
        return [core * half]
    chip = lax.axis_index("group") // 2
    rows = half // chips
    return [(2 * traced_partner(chip, k, chips) + core) * rows for k in range(chips)]


def take_half(ref, spread, core, chips, groups):
    half = ref.shape[1]
    rows = half // chips
    for k, first in enumerate(pieces_of(core, chips, groups, half)):
        ref[:, pl.ds(k * rows, rows)] = spread[:, pl.ds(pl.multiple_of(first, BLOCK), rows)]


def root_term_kernel(chips, groups, *refs):
    map_ref, own_ref = refs[:2]
    arrived = refs[2:-3]
    mine_ref, other_ref, spread = refs[-3:]
    core = lax.axis_index("group") & 1
    spread[...] = jnp.zeros_like(spread)
    for i in range(own_ref.shape[1] // BLOCK):
        total = own_ref[:, static_block(i)]
        for term in arrived:
            total = total + term[:, static_block(i)].astype(F32)
        spread[:, at_block(map_ref[0, 0, i])] = total.astype(BF16)
    take_half(other_ref, spread, 1 - core, chips, groups)
    take_half(mine_ref, spread, core, chips, groups)


def join(joined, mine_ref, other_ref, chips, groups):
    core = lax.axis_index("group") & 1
    half = mine_ref.shape[1]
    rows = half // chips
    for ref, owner in ((mine_ref, core), (other_ref, 1 - core)):
        for k, first in enumerate(pieces_of(owner, chips, groups, half)):
            joined[:, pl.ds(pl.multiple_of(first, BLOCK), rows)] = ref[:, pl.ds(k * rows, rows)]


def root_forward_kernel(chips, groups, mine_ref, other_ref, inverse_ref, out_ref, joined):
    join(joined, mine_ref, other_ref, chips, groups)
    out_ref[...] = times_transpose(joined[...], inverse_ref[...]).astype(BF16)


def root_back_kernel(chips, groups, inverse_ref, forward_ref, mine_ref, other_ref, spread):
    core = lax.axis_index("group") & 1
    spread[...] = times(forward_ref[...], inverse_ref[...]).astype(BF16)
    take_half(other_ref, spread, 1 - core, chips, groups)
    take_half(mine_ref, spread, core, chips, groups)


def root_pick_kernel(chips, groups, map_ref, mine_ref, other_ref, values_ref, joined):
    join(joined, mine_ref, other_ref, chips, groups)
    for i in range(values_ref.shape[1] // BLOCK):
        values_ref[:, static_block(i)] = joined[:, at_block(map_ref[0, 0, i])]


def root_out_kernel(total_ref, out_ref):
    out_ref[0] = total_ref[...].astype(F32).T.astype(BF16)


def root_slice_kernel(mine_ref, other_ref, out_ref, joined, turned):
    join(joined, mine_ref, other_ref, 1, 0)
    rows_out = out_ref.shape[1]
    first = lax.axis_index("group") * rows_out
    turned[...] = joined[:, at_block(first // BLOCK)].astype(F32).T
    begin = pl.multiple_of(lax.rem(first, jnp.int32(BLOCK)), rows_out)
    out_ref[0] = turned[pl.ds(begin, rows_out), :].astype(BF16)


def mid_back_kernel(members, *refs):
    map_ref, inverse_ref, border_ref, forward_ref = refs[:4]
    values = refs[4 : 4 + members]
    outs = refs[4 + members : -1]
    base_ref, own_ref = outs[:2]
    asked_refs = outs[2 : 1 + members]
    piece_refs = outs[1 + members :]
    part = refs[-1]
    member = lax.axis_index("member")
    pivot_blocks = part.shape[1] // BLOCK
    rows = values[0].shape[1]
    back = forward_ref[...].astype(F32)
    for k, ref in enumerate(values):
        owner = traced_source(member, k, members)
        piece = border_ref[0, pl.ds(pl.multiple_of(owner * rows, BLOCK), rows), :]
        back = back - times(ref[...], piece)
    part[...] = times(back.astype(BF16), inverse_ref[0]).astype(BF16)
    blocks = base_ref.shape[1] // BLOCK
    for k, ref in enumerate(asked_refs, start=1):
        owner = traced_partner(member, k, members)
        for j in range(blocks):
            target = map_ref[0, owner, j]
            inside = target < pivot_blocks

            @pl.when(inside)
            def _():
                ref[:, static_block(j)] = part[:, at_block(target)]

            @pl.when(jnp.logical_not(inside))
            def _():
                ref[:, static_block(j)] = jnp.zeros((ref.shape[0], BLOCK), BF16)

    for j in range(blocks):
        target = map_ref[0, member, j]

        @pl.when(target < pivot_blocks)
        def _():
            base_ref[:, static_block(j)] = part[:, at_block(target)]

        border = target - pivot_blocks
        for k, values_ref in enumerate(values):
            inner = border - traced_source(member, k, members) * (rows // BLOCK)

            @pl.when((border >= 0) & (inner >= 0) & (inner < rows // BLOCK))
            def _():
                base_ref[:, static_block(j)] = values_ref[:, at_block(inner)]

    size = own_ref.shape[1]
    own_ref[...] = part[:, at_part(member, size)]
    for k, ref in enumerate(piece_refs, start=1):
        ref[...] = part[:, at_part(traced_partner(member, k, members), size)]


def leaf_back_kernel(*refs):
    factor_ref, edge_ref, forward_ref = refs[:3]
    terms = refs[3:-1]
    out_ref = refs[-1]
    picked = terms[0][...].astype(F32)
    for term in terms[1:]:
        picked = picked + term[...].astype(F32)
    back = forward_ref[...].astype(F32) - times(picked.astype(BF16), edge_ref[0, 0])
    out_ref[0, 0] = times(back.astype(BF16), factor_ref[0, 0]).T.astype(BF16)


def mid_out_kernel(*refs):
    total = refs[0][...].astype(F32)
    for term in refs[1:-1]:
        total = total + term[...].astype(F32)
    refs[-1][0] = total.T.astype(BF16)


def call(kernel, name, inputs, outs, scratch=(), flops=0):
    vmem = pl.BlockSpec(memory_space=pltpu.VMEM)
    smem = pl.BlockSpec(memory_space=pltpu.SMEM)
    moved = sum(x.size * x.dtype.itemsize for x in inputs)
    return pl.pallas_call(
        kernel,
        name=name,
        in_specs=[smem if x.dtype == jnp.int32 else vmem for x in inputs],
        out_specs=[vmem] * len(outs),
        out_shape=[jax.ShapeDtypeStruct(shape, dtype) for shape, dtype in outs],
        scratch_shapes=list(scratch),
        compiler_params=pltpu.CompilerParams(vmem_limit_bytes=VMEM_LIMIT),
        cost_estimate=pl.CostEstimate(flops=flops, bytes_accessed=moved, transcendentals=0),
    )(*inputs)


def total_of(first, others):
    total = first.astype(F32)
    for other in others:
        total = total + other.astype(F32)
    return total.astype(BF16)


def chips_of(groups, rows_out):
    return groups // 2 if rows_out % BLOCK == 0 and groups > 2 else 1


def group_sum(mine, other, size, chips):
    received = exchange(other, "group", 1, size)
    steps = range(2, size, 2)
    if chips == 1:
        piece = total_of(mine, [received])
        mine = piece = total_of(piece, [exchange(piece, "group", k, size) for k in steps])
    else:
        rows = mine.shape[1] // chips
        parts = [
            total_of(mine[:, k * rows : (k + 1) * rows], [received[:, k * rows : (k + 1) * rows]])
            for k in range(chips)
        ]
        arrived = [exchange(part, "group", k, size) for k, part in zip(steps, parts[1:])]
        piece = total_of(parts[0], arrived)
        mine = jnp.concatenate(
            [piece] + [exchange(piece, "group", k, size) for k in steps], axis=1
        )
    return piece, mine, exchange(mine, "group", 1, size)


def member_sum(values, size):
    if not is_power_of_two(size):
        return lax.psum(values, "member")
    rows = values.shape[1] // 2
    low, high = values[:, :rows], values[:, rows:]
    steps = [1 << i for i in range(size.bit_length() - 1)]
    for first, second in zip(steps, reversed(steps)):
        other_low = exchange(low, "member", first, size)
        other_high = exchange(high, "member", second, size)
        low, high = total_of(low, [other_low]), total_of(high, [other_high])
    return jnp.concatenate([low, high], axis=1)


def make_on_device(groups, members):
    steps = range(1, members)

    def on_device(
        rhs,
        leaf_pivot_inverse,
        leaf_border_block,
        leaf_map,
        mid_inverse,
        mid_border,
        root_map,
        root_inverse,
    ):
        columns = rhs.shape[3]
        leaf_pivots = rhs.shape[2]
        leaf_rows = leaf_border_block.shape[2]
        own_pivots, pivots = mid_inverse.shape[1:]
        border_rows = mid_border.shape[1]
        own_border = border_rows // members
        row_count, share_rows = root_inverse.shape
        half = share_rows // 2
        rows_out = share_rows // groups

        def flat(rows, dtype=BF16):
            return ((columns, rows), dtype)

        def spread_over_members(values):
            return [values] + [exchange(values, "member", k, members) for k in steps]

        leaf_forward, leaf_out = call(
            leaf_forward_kernel,
            "leaf_forward",
            [rhs, leaf_pivot_inverse, leaf_border_block],
            [flat(leaf_pivots), flat(leaf_rows)],
            flops=2 * columns * leaf_pivots * (leaf_pivots + leaf_rows),
        )
        terms = spread_over_members(leaf_out)
        mid_forward, *sent = call(
            functools.partial(mid_forward_kernel, members),
            "mid_forward",
            [leaf_map, mid_inverse, mid_border, *terms],
            [flat(own_pivots)] + [flat(own_border)] * len(steps),
            [pltpu.VMEM((columns, pivots), F32)],
            flops=2 * columns * own_pivots * (pivots + border_rows),
        )
        arrived = [exchange(piece, "member", k, members) for k, piece in zip(steps, sent)]
        (own_update,) = call(
            functools.partial(own_update_kernel, members, pivots // BLOCK),
            "own_update",
            [leaf_map, mid_border, mid_forward, *terms],
            [flat(own_border, F32)],
            flops=2 * columns * own_pivots * own_border,
        )
        chips = chips_of(groups, rows_out)
        whole_share = pltpu.VMEM((columns, share_rows), BF16)
        mine, other = call(
            functools.partial(root_term_kernel, chips, groups),
            "root_term",
            [root_map, own_update, *arrived],
            [flat(half), flat(half)],
            [whole_share],
        )
        _, mine, other = group_sum(mine, other, groups, chips)
        (root_part,) = call(
            functools.partial(root_forward_kernel, chips, groups),
            "root_forward",
            [mine, other, root_inverse],
            [flat(row_count)],
            [whole_share],
            flops=2 * columns * row_count * share_rows,
        )
        mine, other = call(
            functools.partial(root_back_kernel, chips, groups),
            "root_back",
            [root_inverse, member_sum(root_part, members)],
            [flat(half), flat(half)],
            [whole_share],
            flops=2 * columns * row_count * share_rows,
        )
        piece, mine, other = group_sum(mine, other, groups, chips)
        (own_values,) = call(
            functools.partial(root_pick_kernel, chips, groups),
            "root_pick",
            [root_map, mine, other],
            [flat(own_border)],
            [whole_share],
        )
        shape = [((1, rows_out, columns), BF16)]
        if chips > 1:
            (root_out,) = call(root_out_kernel, "root_out", [piece], shape)
        else:
            (root_out,) = call(
                root_slice_kernel,
                "root_slice",
                [mine, other],
                shape,
                [whole_share, pltpu.VMEM((BLOCK, columns), F32)],
            )
        base, own_piece, *sent = call(
            functools.partial(mid_back_kernel, members),
            "mid_back",
            [leaf_map, mid_inverse, mid_border, mid_forward, *spread_over_members(own_values)],
            [flat(leaf_rows), flat(own_pivots)]
            + [flat(leaf_rows)] * len(steps)
            + [flat(own_pivots)] * len(steps),
            [pltpu.VMEM((columns, pivots), BF16)],
            flops=2 * columns * own_pivots * (pivots + border_rows),
        )
        asked, pieces = sent[: len(steps)], sent[len(steps) :]
        picked = [exchange(part, "member", k, members) for k, part in zip(steps, asked)]
        (leaf_values,) = call(
            leaf_back_kernel,
            "leaf_back",
            [leaf_pivot_inverse, leaf_border_block, leaf_forward, base, *picked],
            [((1, 1, leaf_pivots, columns), BF16)],
            flops=2 * columns * leaf_pivots * (leaf_pivots + leaf_rows),
        )
        pieces = [exchange(part, "member", k, members) for k, part in zip(steps, pieces)]
        (mid_out,) = call(
            mid_out_kernel, "mid_out", [own_piece, *pieces], [((1, own_pivots, columns), BF16)]
        )
        return leaf_values, mid_out, root_out

    return on_device


def solution(mesh):
    in_specs = (
        P("group", "member", None, None),
        P("group", "member", None, None),
        P("group", "member", None, None),
        P("group", None, None),
        P("group", "member", None),
        P("group", None, "member"),
        P("group", "member", None),
        P("group", "member"),
    )
    out_specs = (
        P("group", "member", None, None),
        P("group", "member", None),
        P("member", "group", None),
    )
    on_device = make_on_device(mesh.shape["group"], mesh.shape["member"])
    return jax.shard_map(
        on_device, mesh=mesh, in_specs=in_specs, out_specs=out_specs, check_vma=False
    )
```

```python
import functools

import jax
import jax.numpy as jnp
from jax import lax
from jax.experimental import pallas as pl
from jax.experimental.pallas import tpu as pltpu
from jax.sharding import PartitionSpec as P

BLOCK = 128
VMEM_LIMIT = 20 * 1024 * 1024
PREFETCH_FLOPS = 2 * 10**10
F32 = jnp.float32
BF16 = jnp.bfloat16


def is_power_of_two(size):
    return size & (size - 1) == 0


def partner(index, step, size):
    return index ^ step if is_power_of_two(size) else (index + step) % size


def source(index, step, size):
    return index ^ step if is_power_of_two(size) else (index - step) % size


def exchange(values, axis, step, size):
    return lax.ppermute(values, axis, [(i, partner(i, step, size)) for i in range(size)])


def times_transpose(values, matrix):
    return lax.dot_general(values, matrix, (((1,), (1,)), ((), ())), preferred_element_type=F32)


def times(values, matrix):
    return jnp.dot(values, matrix, preferred_element_type=F32)


def traced_source(index, step, size):
    if is_power_of_two(size):
        return lax.bitwise_xor(index, jnp.int32(step))
    return lax.rem(index - step + size, jnp.int32(size))


def traced_partner(index, step, size):
    if is_power_of_two(size):
        return lax.bitwise_xor(index, jnp.int32(step))
    return lax.rem(index + step, jnp.int32(size))


def at_block(index):
    return pl.ds(pl.multiple_of(index * BLOCK, BLOCK), BLOCK)


def at_part(index, size):
    return pl.ds(pl.multiple_of(index * size, BLOCK), size)


def static_block(index):
    return pl.ds(index * BLOCK, BLOCK)


def chunks_of(size):
    rows = 2 * BLOCK if size % (2 * BLOCK) == 0 else size
    return [(first, rows) for first in range(0, size, rows)]


def leaf_forward_kernel(
    rhs_hbm, factor_hbm, edge_hbm, forward_ref, factor_ref, edge_ref, rhs_ref, sems
):
    chunks = chunks_of(factor_ref.shape[0])
    copies = [pltpu.make_async_copy(rhs_hbm.at[0, 0], rhs_ref, sems.at[0])]
    for i, (first, rows) in enumerate(chunks, start=1):
        part = (pl.ds(first, rows), pl.ds(0, first + rows))
        copies.append(
            pltpu.make_async_copy(factor_hbm.at[0, 0, *part], factor_ref.at[*part], sems.at[i])
        )
    edge_copy = pltpu.make_async_copy(edge_hbm.at[0, 0], edge_ref, sems.at[1 + len(chunks)])
    for copy in copies:
        copy.start()
    edge_copy.start()
    copies[0].wait()
    source_rows = rhs_ref[...].T
    for copy, (first, rows) in zip(copies[1:], chunks):
        copy.wait()
        factor = factor_ref[pl.ds(first, rows), pl.ds(0, first + rows)]
        forward = times_transpose(source_rows[:, : first + rows], factor)
        forward_ref[:, pl.ds(first, rows)] = forward.astype(BF16)
    edge_copy.wait()


def leaf_out_kernel(forward_ref, edge_ref, out_ref):
    out_ref[...] = (-times_transpose(forward_ref[...], edge_ref[...])).astype(BF16)


def border_piece(border_ref, owner, rows):
    return border_ref[0, pl.ds(pl.multiple_of(owner * rows, BLOCK), rows), :]


def mid_forward_kernel(members, map_ref, inverse_ref, *refs):
    terms = refs[:members]
    forward_ref, front = refs[members:]
    member = lax.axis_index("member")
    pivot_blocks = front.shape[1] // BLOCK
    front[...] = jnp.zeros_like(front)
    for k, term in enumerate(terms):
        owner = traced_source(member, k, members)
        for j in range(term.shape[1] // BLOCK):
            target = map_ref[0, owner, j]

            @pl.when(target < pivot_blocks)
            def _():
                front[:, at_block(target)] += term[:, static_block(j)].astype(F32)

    forward_ref[...] = times_transpose(front[...].astype(BF16), inverse_ref[0]).astype(BF16)


def mid_piece_kernel(members, step, border_ref, forward_ref, out_ref):
    owner = traced_partner(lax.axis_index("member"), step, members)
    piece = border_piece(border_ref, owner, out_ref.shape[1])
    out_ref[...] = (-times_transpose(forward_ref[...], piece)).astype(BF16)


def own_update_kernel(members, pivot_blocks, *refs):
    map_ref, border_ref, forward_ref = refs[:3]
    terms = refs[3 : 3 + members]
    update_ref = refs[-1]
    member = lax.axis_index("member")
    rows = update_ref.shape[1]
    piece = border_ref[0, pl.ds(pl.multiple_of(member * rows, BLOCK), rows), :]
    update_ref[...] = -times_transpose(forward_ref[...], piece)
    first = pivot_blocks + member * (rows // BLOCK)
    for k, term in enumerate(terms):
        owner = traced_source(member, k, members)
        for j in range(term.shape[1] // BLOCK):
            target = map_ref[0, owner, j] - first

            @pl.when((target >= 0) & (target < rows // BLOCK))
            def _():
                update_ref[:, at_block(target)] += term[:, static_block(j)].astype(F32)


def pieces_of(core, chips, groups, half):
    if chips == 1:
        return [core * half]
    chip = lax.axis_index("group") // 2
    rows = half // chips
    return [(2 * traced_partner(chip, k, chips) + core) * rows for k in range(chips)]


def take_half(ref, spread, core, chips, groups):
    half = ref.shape[1]
    rows = half // chips
    for k, first in enumerate(pieces_of(core, chips, groups, half)):
        ref[:, pl.ds(k * rows, rows)] = spread[:, pl.ds(pl.multiple_of(first, BLOCK), rows)]


def root_term_kernel(chips, groups, *refs):
    map_ref, own_ref = refs[:2]
    arrived = refs[2:-3]
    mine_ref, other_ref, spread = refs[-3:]
    core = lax.axis_index("group") & 1
    spread[...] = jnp.zeros_like(spread)
    for i in range(own_ref.shape[1] // BLOCK):
        total = own_ref[:, static_block(i)]
        for term in arrived:
            total = total + term[:, static_block(i)].astype(F32)
        spread[:, at_block(map_ref[0, 0, i])] = total.astype(BF16)
    take_half(other_ref, spread, 1 - core, chips, groups)
    take_half(mine_ref, spread, core, chips, groups)


def join(joined, mine_ref, other_ref, chips, groups):
    core = lax.axis_index("group") & 1
    half = mine_ref.shape[1]
    rows = half // chips
    for ref, owner in ((mine_ref, core), (other_ref, 1 - core)):
        for k, first in enumerate(pieces_of(owner, chips, groups, half)):
            joined[:, pl.ds(pl.multiple_of(first, BLOCK), rows)] = ref[:, pl.ds(k * rows, rows)]


def root_half(chips, groups, owner, half_ref, inverse_ref):
    half = half_ref.shape[1]
    rows = half // chips
    total = None
    for k, first in enumerate(pieces_of(owner, chips, groups, half)):
        columns = inverse_ref[:, pl.ds(pl.multiple_of(first, BLOCK), rows)]
        part = times_transpose(half_ref[:, pl.ds(k * rows, rows)], columns)
        total = part if total is None else total + part
    return total


def root_own_kernel(chips, groups, mine_ref, inverse_ref, out_ref):
    core = lax.axis_index("group") & 1
    out_ref[...] = root_half(chips, groups, core, mine_ref, inverse_ref)


def root_forward_kernel(chips, groups, own_ref, other_ref, inverse_ref, out_ref):
    core = lax.axis_index("group") & 1
    total = own_ref[...] + root_half(chips, groups, 1 - core, other_ref, inverse_ref)
    out_ref[...] = total.astype(BF16)


def root_back_kernel(chips, groups, own, inverse_ref, forward_ref, half_ref):
    core = lax.axis_index("group") & 1
    half = half_ref.shape[1]
    rows = half // chips
    forward = forward_ref[...]
    for k, first in enumerate(pieces_of(core if own else 1 - core, chips, groups, half)):
        columns = inverse_ref[:, pl.ds(pl.multiple_of(first, BLOCK), rows)]
        half_ref[:, pl.ds(k * rows, rows)] = times(forward, columns).astype(BF16)


def root_pick_kernel(chips, groups, map_ref, mine_ref, other_ref, values_ref, joined):
    join(joined, mine_ref, other_ref, chips, groups)
    for i in range(values_ref.shape[1] // BLOCK):
        values_ref[:, static_block(i)] = joined[:, at_block(map_ref[0, 0, i])]


def root_out_kernel(total_ref, out_ref):
    out_ref[0] = total_ref[...].astype(F32).T.astype(BF16)


def root_slice_kernel(mine_ref, other_ref, out_ref, joined, turned):
    join(joined, mine_ref, other_ref, 1, 0)
    rows_out = out_ref.shape[1]
    first = lax.axis_index("group") * rows_out
    turned[...] = joined[:, at_block(first // BLOCK)].astype(F32).T
    begin = pl.multiple_of(lax.rem(first, jnp.int32(BLOCK)), rows_out)
    out_ref[0] = turned[pl.ds(begin, rows_out), :].astype(BF16)


def mid_early_kernel(members, early, border_ref, forward_ref, *refs):
    back = forward_ref[...].astype(F32)
    member = lax.axis_index("member")
    for k, ref in zip(early, refs):
        owner = traced_source(member, k, members)
        back = back - times(ref[...], border_piece(border_ref, owner, ref.shape[1]))
    refs[-1][...] = back


def mid_back_kernel(members, late, *refs):
    map_ref, inverse_ref, border_ref, forward_ref = refs[:4]
    values = refs[4 : 4 + members]
    outs = refs[4 + members : -1]
    base_ref, own_ref = outs[:2]
    asked_refs = outs[2 : 1 + members]
    piece_refs = outs[1 + members :]
    part = refs[-1]
    member = lax.axis_index("member")
    pivot_blocks = part.shape[1] // BLOCK
    rows = values[0].shape[1]
    back = forward_ref[...]
    for k in late:
        owner = traced_source(member, k, members)
        back = back - times(values[k][...], border_piece(border_ref, owner, rows))
    part[...] = times(back.astype(BF16), inverse_ref[0]).astype(BF16)
    blocks = base_ref.shape[1] // BLOCK
    for k, ref in enumerate(asked_refs, start=1):
        owner = traced_partner(member, k, members)
        for j in range(blocks):
            target = map_ref[0, owner, j]
            inside = target < pivot_blocks

            @pl.when(inside)
            def _():
                ref[:, static_block(j)] = part[:, at_block(target)]

            @pl.when(jnp.logical_not(inside))
            def _():
                ref[:, static_block(j)] = jnp.zeros((ref.shape[0], BLOCK), BF16)

    for j in range(blocks):
        target = map_ref[0, member, j]

        @pl.when(target < pivot_blocks)
        def _():
            base_ref[:, static_block(j)] = part[:, at_block(target)]

        border = target - pivot_blocks
        for k, values_ref in enumerate(values):
            inner = border - traced_source(member, k, members) * (rows // BLOCK)

            @pl.when((border >= 0) & (inner >= 0) & (inner < rows // BLOCK))
            def _():
                base_ref[:, static_block(j)] = values_ref[:, at_block(inner)]

    size = own_ref.shape[1]
    own_ref[...] = part[:, at_part(member, size)]
    for k, ref in enumerate(piece_refs, start=1):
        ref[...] = part[:, at_part(traced_partner(member, k, members), size)]


def leaf_back_kernel(*refs):
    factor_ref, edge_ref, forward_ref = refs[:3]
    terms = refs[3:-1]
    out_ref = refs[-1]
    picked = terms[0][...].astype(F32)
    for term in terms[1:]:
        picked = picked + term[...].astype(F32)
    back = forward_ref[...].astype(F32) - times(picked.astype(BF16), edge_ref[...])
    back = back.astype(BF16)
    chunks = chunks_of(factor_ref.shape[0])
    for first, rows in chunks:
        total = None
        for lower, size in chunks:
            if lower >= first:
                factor = factor_ref[pl.ds(lower, size), pl.ds(first, rows)]
                part = times(back[:, lower : lower + size], factor)
                total = part if total is None else total + part
        out_ref[0, 0, pl.ds(first, rows), :] = total.T.astype(BF16)


def mid_out_kernel(*refs):
    total = refs[0][...].astype(F32)
    for term in refs[1:-1]:
        total = total + term[...].astype(F32)
    refs[-1][0] = total.T.astype(BF16)


def call(kernel, name, inputs, outs, scratch=(), flops=0, space=pltpu.VMEM):
    vmem = pl.BlockSpec(memory_space=pltpu.VMEM)
    place = pl.BlockSpec(memory_space=space)
    out = jax.ShapeDtypeStruct
    if space == pltpu.HBM:
        inputs = [pltpu.with_memory_space_constraint(x, space) for x in inputs]
        out = pltpu.VMEM
    smem = pl.BlockSpec(memory_space=pltpu.SMEM)
    moved = sum(x.size * x.dtype.itemsize for x in inputs)
    return pl.pallas_call(
        kernel,
        name=name,
        in_specs=[smem if x.dtype == jnp.int32 else place for x in inputs],
        out_specs=[vmem] * len(outs),
        out_shape=[out(shape, dtype) for shape, dtype in outs],
        scratch_shapes=list(scratch),
        compiler_params=pltpu.CompilerParams(vmem_limit_bytes=VMEM_LIMIT),
        cost_estimate=pl.CostEstimate(flops=flops, bytes_accessed=moved, transcendentals=0),
    )(*inputs)


def total_of(first, others):
    total = first.astype(F32)
    for other in others:
        total = total + other.astype(F32)
    return total.astype(BF16)


def chips_of(groups, rows_out):
    return groups // 2 if rows_out % BLOCK == 0 and groups > 2 else 1


def group_sum(mine, other, size, chips):
    received = exchange(other, "group", 1, size)
    steps = range(2, size, 2)
    if chips == 1:
        piece = total_of(mine, [received])
        mine = piece = total_of(piece, [exchange(piece, "group", k, size) for k in steps])
    else:
        rows = mine.shape[1] // chips
        parts = [
            total_of(mine[:, k * rows : (k + 1) * rows], [received[:, k * rows : (k + 1) * rows]])
            for k in range(chips)
        ]
        arrived = [exchange(part, "group", k, size) for k, part in zip(steps, parts[1:])]
        piece = total_of(parts[0], arrived)
        mine = jnp.concatenate(
            [piece] + [exchange(piece, "group", k, size) for k in steps], axis=1
        )
    return piece, mine, exchange(mine, "group", 1, size)


def member_sum(values, size):
    if not is_power_of_two(size):
        return lax.psum(values, "member")
    rows = values.shape[1] // 2
    low, high = values[:, :rows], values[:, rows:]
    steps = [1 << i for i in range(size.bit_length() - 1)]
    for first, second in zip(steps, reversed(steps)):
        other_low = exchange(low, "member", first, size)
        other_high = exchange(high, "member", second, size)
        low, high = total_of(low, [other_low]), total_of(high, [other_high])
    return jnp.concatenate([low, high], axis=1)


def make_on_device(groups, members):
    steps = range(1, members)

    def on_device(
        rhs,
        leaf_pivot_inverse,
        leaf_border_block,
        leaf_map,
        mid_inverse,
        mid_border,
        root_map,
        root_inverse,
    ):
        columns = rhs.shape[3]
        leaf_pivots = rhs.shape[2]
        leaf_rows = leaf_border_block.shape[2]
        own_pivots, pivots = mid_inverse.shape[1:]
        border_rows = mid_border.shape[1]
        own_border = border_rows // members
        row_count, share_rows = root_inverse.shape
        half = share_rows // 2
        rows_out = share_rows // groups

        def flat(rows, dtype=BF16):
            return ((columns, rows), dtype)

        def spread_over_members(values):
            return [values] + [exchange(values, "member", k, members) for k in steps]

        leaf_forward, leaf_factor, leaf_edge = call(
            leaf_forward_kernel,
            "leaf_forward",
            [rhs, leaf_pivot_inverse, leaf_border_block],
            [
                flat(leaf_pivots),
                (leaf_pivot_inverse.shape[2:], BF16),
                (leaf_border_block.shape[2:], BF16),
            ],
            [
                pltpu.VMEM((leaf_pivots, columns), BF16),
                pltpu.SemaphoreType.DMA((2 + len(chunks_of(leaf_pivots)),)),
            ],
            flops=2 * columns * leaf_pivots * leaf_pivots,
            space=pltpu.HBM,
        )
        (leaf_out,) = call(
            leaf_out_kernel,
            "leaf_out",
            [leaf_forward, leaf_edge],
            [flat(leaf_rows)],
            flops=PREFETCH_FLOPS,
        )
        terms = spread_over_members(leaf_out)
        (mid_forward,) = call(
            functools.partial(mid_forward_kernel, members),
            "mid_forward",
            [leaf_map, mid_inverse, *terms],
            [flat(own_pivots)],
            [pltpu.VMEM((columns, pivots), F32)],
            flops=2 * columns * own_pivots * pivots,
        )
        arrived = []
        for k in reversed(steps):
            (piece,) = call(
                functools.partial(mid_piece_kernel, members, k),
                f"mid_piece_{k}",
                [mid_border, mid_forward],
                [flat(own_border)],
                flops=2 * columns * own_pivots * own_border,
            )
            arrived.append(exchange(piece, "member", k, members))
        (own_update,) = call(
            functools.partial(own_update_kernel, members, pivots // BLOCK),
            "own_update",
            [leaf_map, mid_border, mid_forward, *terms],
            [flat(own_border, F32)],
            flops=2 * columns * own_pivots * own_border,
        )
        chips = chips_of(groups, rows_out)
        whole_share = pltpu.VMEM((columns, share_rows), BF16)
        mine, other = call(
            functools.partial(root_term_kernel, chips, groups),
            "root_term",
            [root_map, own_update, *arrived],
            [flat(half), flat(half)],
            [whole_share],
        )
        _, mine, other = group_sum(mine, other, groups, chips)
        root_flops = columns * row_count * share_rows
        (root_own,) = call(
            functools.partial(root_own_kernel, chips, groups),
            "root_own",
            [mine, root_inverse],
            [flat(row_count, F32)],
            flops=root_flops,
        )
        (root_part,) = call(
            functools.partial(root_forward_kernel, chips, groups),
            "root_forward",
            [root_own, other, root_inverse],
            [flat(row_count)],
            flops=root_flops,
        )
        root_forward = member_sum(root_part, members)
        other, mine = (
            call(
                functools.partial(root_back_kernel, chips, groups, own),
                "root_back_own" if own else "root_back_other",
                [root_inverse, root_forward],
                [flat(half)],
                flops=root_flops,
            )[0]
            for own in (False, True)
        )
        piece, mine, other = group_sum(mine, other, groups, chips)
        (own_values,) = call(
            functools.partial(root_pick_kernel, chips, groups),
            "root_pick",
            [root_map, mine, other],
            [flat(own_border)],
            [whole_share],
        )
        shape = [((1, rows_out, columns), BF16)]
        if chips > 1:
            (root_out,) = call(root_out_kernel, "root_out", [piece], shape)
        else:
            (root_out,) = call(
                root_slice_kernel,
                "root_slice",
                [mine, other],
                shape,
                [whole_share, pltpu.VMEM((BLOCK, columns), F32)],
            )
        values = spread_over_members(own_values)
        early = (0,) if members < 3 else (0, members - 1)
        late = tuple(k for k in range(members) if k not in early)
        (mid_early,) = call(
            functools.partial(mid_early_kernel, members, early),
            "mid_early",
            [mid_border, mid_forward] + [values[k] for k in early],
            [flat(own_pivots, F32)],
            flops=2 * columns * own_pivots * own_border * len(early),
        )
        base, own_piece, *sent = call(
            functools.partial(mid_back_kernel, members, late),
            "mid_back",
            [leaf_map, mid_inverse, mid_border, mid_early, *values],
            [flat(leaf_rows), flat(own_pivots)]
            + [flat(leaf_rows)] * len(steps)
            + [flat(own_pivots)] * len(steps),
            [pltpu.VMEM((columns, pivots), BF16)],
            flops=2 * columns * own_pivots * (pivots + border_rows),
        )
        asked, pieces = sent[: len(steps)], sent[len(steps) :]
        picked = [exchange(part, "member", k, members) for k, part in zip(steps, asked)]
        (leaf_values,) = call(
            leaf_back_kernel,
            "leaf_back",
            [leaf_factor, leaf_edge, leaf_forward, base, *picked],
            [((1, 1, leaf_pivots, columns), BF16)],
            flops=2 * columns * leaf_pivots * (leaf_pivots + leaf_rows),
        )
        pieces = [exchange(part, "member", k, members) for k, part in zip(steps, pieces)]
        (mid_out,) = call(
            mid_out_kernel, "mid_out", [own_piece, *pieces], [((1, own_pivots, columns), BF16)]
        )
        return leaf_values, mid_out, root_out

    return on_device


def solution(mesh):
    in_specs = (
        P("group", "member", None, None),
        P("group", "member", None, None),
        P("group", "member", None, None),
        P("group", None, None),
        P("group", "member", None),
        P("group", None, "member"),
        P("group", "member", None),
        P("group", "member"),
    )
    out_specs = (
        P("group", "member", None, None),
        P("group", "member", None),
        P("member", "group", None),
    )
    on_device = make_on_device(mesh.shape["group"], mesh.shape["member"])
    return jax.shard_map(
        on_device, mesh=mesh, in_specs=in_specs, out_specs=out_specs, check_vma=False
    )
```

```python
import functools

import jax
import jax.numpy as jnp
from jax import lax
from jax.experimental import pallas as pl
from jax.experimental.pallas import tpu as pltpu
from jax.sharding import PartitionSpec as P

BLOCK = 128
VMEM_LIMIT = 20 * 1024 * 1024
PREFETCH_FLOPS = 2 * 10**10
F32 = jnp.float32
BF16 = jnp.bfloat16


def is_power_of_two(size):
    return size & (size - 1) == 0


def partner(index, step, size):
    return index ^ step if is_power_of_two(size) else (index + step) % size


def source(index, step, size):
    return index ^ step if is_power_of_two(size) else (index - step) % size


def exchange(values, axis, step, size):
    return lax.ppermute(values, axis, [(i, partner(i, step, size)) for i in range(size)])


def times_transpose(values, matrix):
    return lax.dot_general(values, matrix, (((1,), (1,)), ((), ())), preferred_element_type=F32)


def times(values, matrix):
    return jnp.dot(values, matrix, preferred_element_type=F32)


def traced_source(index, step, size):
    if is_power_of_two(size):
        return lax.bitwise_xor(index, jnp.int32(step))
    return lax.rem(index - step + size, jnp.int32(size))


def traced_partner(index, step, size):
    if is_power_of_two(size):
        return lax.bitwise_xor(index, jnp.int32(step))
    return lax.rem(index + step, jnp.int32(size))


def at_block(index):
    return pl.ds(pl.multiple_of(index * BLOCK, BLOCK), BLOCK)


def at_part(index, size):
    return pl.ds(pl.multiple_of(index * size, BLOCK), size)


def static_block(index):
    return pl.ds(index * BLOCK, BLOCK)


def chunks_of(size):
    rows = 2 * BLOCK if size % (2 * BLOCK) == 0 else size
    return [(first, rows) for first in range(0, size, rows)]


def leaf_forward_kernel(
    rhs_hbm, factor_hbm, edge_hbm, forward_ref, factor_ref, edge_ref, rhs_ref, sems
):
    chunks = chunks_of(factor_ref.shape[0])
    copies = [pltpu.make_async_copy(rhs_hbm.at[0, 0], rhs_ref, sems.at[0])]
    for i, (first, rows) in enumerate(chunks, start=1):
        part = (pl.ds(first, rows), pl.ds(0, first + rows))
        copies.append(
            pltpu.make_async_copy(factor_hbm.at[0, 0, *part], factor_ref.at[*part], sems.at[i])
        )
    edge_copy = pltpu.make_async_copy(edge_hbm.at[0, 0], edge_ref, sems.at[1 + len(chunks)])
    for copy in copies:
        copy.start()
    edge_copy.start()
    copies[0].wait()
    source_rows = rhs_ref[...].T
    for copy, (first, rows) in zip(copies[1:], chunks):
        copy.wait()
        factor = factor_ref[pl.ds(first, rows), pl.ds(0, first + rows)]
        forward = times_transpose(source_rows[:, : first + rows], factor)
        forward_ref[:, pl.ds(first, rows)] = forward.astype(BF16)
    edge_copy.wait()


def leaf_out_kernel(forward_ref, edge_ref, out_ref):
    out_ref[...] = (-times_transpose(forward_ref[...], edge_ref[...])).astype(BF16)


def border_piece(border_ref, owner, rows):
    return border_ref[0, pl.ds(pl.multiple_of(owner * rows, BLOCK), rows), :]


def mid_forward_kernel(members, which, map_ref, inverse_ref, *refs):
    forward_ref, total = refs[-2:]
    terms = refs[: len(which)]
    before = refs[len(which) : -2]
    pivot_blocks = inverse_ref.shape[2] // BLOCK
    member = lax.axis_index("member")
    total[...] = before[0][...] if before else jnp.zeros_like(total)
    for k, term in zip(which, terms):
        owner = traced_source(member, k, members)
        for j in range(term.shape[1] // BLOCK):
            target = map_ref[0, owner, j]

            @pl.when(target < pivot_blocks)
            def _():
                columns = inverse_ref[0, :, at_block(target)]
                total[...] += times_transpose(term[:, static_block(j)], columns)

    forward_ref[...] = total[...].astype(forward_ref.dtype)


def mid_piece_kernel(members, step, border_ref, forward_ref, low_ref, high_ref):
    owner = traced_partner(lax.axis_index("member"), step, members)
    rows = low_ref.shape[1]
    for half, ref in enumerate((low_ref, high_ref)):
        piece = border_piece(border_ref, 2 * owner + half, rows)
        ref[...] = (-times_transpose(forward_ref[...], piece)).astype(BF16)


def own_update_kernel(members, pivot_blocks, *refs):
    map_ref, border_ref, forward_ref = refs[:3]
    terms = refs[3 : 3 + members]
    update_ref = refs[-1]
    member = lax.axis_index("member")
    rows = update_ref.shape[1]
    piece = border_ref[0, pl.ds(pl.multiple_of(member * rows, BLOCK), rows), :]
    update_ref[...] = -times_transpose(forward_ref[...], piece)
    first = pivot_blocks + member * (rows // BLOCK)
    for k, term in enumerate(terms):
        owner = traced_source(member, k, members)
        for j in range(term.shape[1] // BLOCK):
            target = map_ref[0, owner, j] - first

            @pl.when((target >= 0) & (target < rows // BLOCK))
            def _():
                update_ref[:, at_block(target)] += term[:, static_block(j)].astype(F32)


def pieces_of(core, chips, groups, half):
    if chips == 1:
        return [core * half]
    chip = lax.axis_index("group") // 2
    rows = half // chips
    return [(2 * traced_partner(chip, k, chips) + core) * rows for k in range(chips)]


def take_half(ref, spread, core, chips, groups):
    half = ref.shape[1]
    rows = half // chips
    for k, first in enumerate(pieces_of(core, chips, groups, half)):
        ref[:, pl.ds(k * rows, rows)] = spread[:, pl.ds(pl.multiple_of(first, BLOCK), rows)]


def root_term_kernel(chips, groups, lows, *refs):
    map_ref, own_ref = refs[:2]
    arrived = (refs[2 : 2 + lows], refs[2 + lows : -3])
    mine_ref, other_ref, spread = refs[-3:]
    core = lax.axis_index("group") & 1
    spread[...] = jnp.zeros_like(spread)
    half_blocks = own_ref.shape[1] // (2 * BLOCK)
    for i in range(2 * half_blocks):
        total = own_ref[:, static_block(i)]
        for term in arrived[i // half_blocks]:
            total = total + term[:, static_block(i % half_blocks)].astype(F32)
        spread[:, at_block(map_ref[0, 0, i])] = total.astype(BF16)
    take_half(other_ref, spread, 1 - core, chips, groups)
    take_half(mine_ref, spread, core, chips, groups)


def join(joined, mine_ref, other_ref, chips, groups):
    core = lax.axis_index("group") & 1
    half = mine_ref.shape[1]
    rows = half // chips
    for ref, owner in ((mine_ref, core), (other_ref, 1 - core)):
        for k, first in enumerate(pieces_of(owner, chips, groups, half)):
            joined[:, pl.ds(pl.multiple_of(first, BLOCK), rows)] = ref[:, pl.ds(k * rows, rows)]


def root_half(chips, groups, owner, half_ref, inverse_ref):
    half = half_ref.shape[1]
    rows = half // chips
    total = None
    for k, first in enumerate(pieces_of(owner, chips, groups, half)):
        columns = inverse_ref[:, pl.ds(pl.multiple_of(first, BLOCK), rows)]
        part = times_transpose(half_ref[:, pl.ds(k * rows, rows)], columns)
        total = part if total is None else total + part
    return total


def root_own_kernel(chips, groups, mine_ref, inverse_ref, out_ref):
    core = lax.axis_index("group") & 1
    out_ref[...] = root_half(chips, groups, core, mine_ref, inverse_ref)


def root_forward_kernel(chips, groups, own_ref, other_ref, inverse_ref, out_ref):
    core = lax.axis_index("group") & 1
    total = own_ref[...] + root_half(chips, groups, 1 - core, other_ref, inverse_ref)
    out_ref[...] = total.astype(BF16)


def root_back_kernel(chips, groups, own, inverse_ref, forward_ref, half_ref):
    core = lax.axis_index("group") & 1
    half = half_ref.shape[1]
    rows = half // chips
    forward = forward_ref[...]
    for k, first in enumerate(pieces_of(core if own else 1 - core, chips, groups, half)):
        columns = inverse_ref[:, pl.ds(pl.multiple_of(first, BLOCK), rows)]
        half_ref[:, pl.ds(k * rows, rows)] = times(forward, columns).astype(BF16)


def root_pick_kernel(chips, groups, map_ref, mine_ref, other_ref, low_ref, high_ref, joined):
    join(joined, mine_ref, other_ref, chips, groups)
    blocks = low_ref.shape[1] // BLOCK
    for i in range(2 * blocks):
        ref = (low_ref, high_ref)[i // blocks]
        ref[:, static_block(i % blocks)] = joined[:, at_block(map_ref[0, 0, i])]


def root_out_kernel(total_ref, out_ref):
    out_ref[0] = total_ref[...].astype(F32).T.astype(BF16)


def root_slice_kernel(mine_ref, other_ref, out_ref, joined, turned):
    join(joined, mine_ref, other_ref, 1, 0)
    rows_out = out_ref.shape[1]
    first = lax.axis_index("group") * rows_out
    turned[...] = joined[:, at_block(first // BLOCK)].astype(F32).T
    begin = pl.multiple_of(lax.rem(first, jnp.int32(BLOCK)), rows_out)
    out_ref[0] = turned[pl.ds(begin, rows_out), :].astype(BF16)


def border_product(members, values, which, border_ref):
    member = lax.axis_index("member")
    total = None
    for (step, half), ref in zip(which, values):
        owner = traced_source(member, step, members)
        piece = border_piece(border_ref, 2 * owner + half, ref.shape[1])
        part = times(ref[...], piece)
        total = part if total is None else total + part
    return total


def mid_early_kernel(members, which, border_ref, back_ref, *refs):
    product = border_product(members, refs[:-1], which, border_ref)
    refs[-1][...] = back_ref[...].astype(F32) - product


def ask(map_ref, owner, part_ref, out_ref):
    pivot_blocks = part_ref.shape[1] // BLOCK
    for j in range(out_ref.shape[1] // BLOCK):
        target = map_ref[0, owner, j]
        inside = target < pivot_blocks

        @pl.when(inside)
        def _():
            out_ref[:, static_block(j)] = part_ref[:, at_block(target)]

        @pl.when(jnp.logical_not(inside))
        def _():
            out_ref[:, static_block(j)] = jnp.zeros((out_ref.shape[0], BLOCK), BF16)


def mid_back_kernel(members, late, map_ref, inverse_ref, border_ref, back_ref, *refs):
    values = refs[:-3]
    part_ref, asked_ref, piece_ref = refs[-3:]
    back = back_ref[...] - border_product(members, values, late, border_ref)
    part_ref[...] = times(back.astype(BF16), inverse_ref[0]).astype(BF16)
    owner = traced_partner(lax.axis_index("member"), members - 1, members)
    ask(map_ref, owner, part_ref, asked_ref)
    piece_ref[...] = part_ref[:, at_part(owner, piece_ref.shape[1])]


def mid_share_kernel(members, step, map_ref, part_ref, asked_ref, piece_ref):
    owner = traced_partner(lax.axis_index("member"), step, members)
    ask(map_ref, owner, part_ref, asked_ref)
    piece_ref[...] = part_ref[:, at_part(owner, piece_ref.shape[1])]


def pick_kernel(members, map_ref, part_ref, *refs):
    values = refs[:-2]
    base_ref, own_ref = refs[-2:]
    member = lax.axis_index("member")
    pivot_blocks = part_ref.shape[1] // BLOCK
    rows = values[0].shape[1]
    for j in range(base_ref.shape[1] // BLOCK):
        target = map_ref[0, member, j]

        @pl.when(target < pivot_blocks)
        def _():
            base_ref[:, static_block(j)] = part_ref[:, at_block(target)]

        border = target - pivot_blocks
        for k, values_ref in enumerate(values):
            owner = traced_source(member, k // 2, members)
            inner = border - (2 * owner + k % 2) * (rows // BLOCK)

            @pl.when((border >= 0) & (inner >= 0) & (inner < rows // BLOCK))
            def _():
                base_ref[:, static_block(j)] = values_ref[:, at_block(inner)]

    own_ref[...] = part_ref[:, at_part(member, own_ref.shape[1])]


def leaf_back_kernel(*refs):
    factor_ref, edge_ref, forward_ref = refs[:3]
    terms = refs[3:-1]
    out_ref = refs[-1]
    picked = terms[0][...].astype(F32)
    for term in terms[1:]:
        picked = picked + term[...].astype(F32)
    back = forward_ref[...].astype(F32) - times(picked.astype(BF16), edge_ref[...])
    back = back.astype(BF16)
    chunks = chunks_of(factor_ref.shape[0])
    for first, rows in chunks:
        total = None
        for lower, size in chunks:
            if lower >= first:
                factor = factor_ref[pl.ds(lower, size), pl.ds(first, rows)]
                part = times(back[:, lower : lower + size], factor)
                total = part if total is None else total + part
        out_ref[0, 0, pl.ds(first, rows), :] = total.T.astype(BF16)


def mid_out_kernel(*refs):
    total = refs[0][...].astype(F32)
    for term in refs[1:-1]:
        total = total + term[...].astype(F32)
    refs[-1][0] = total.T.astype(BF16)


def call(kernel, name, inputs, outs, scratch=(), flops=0, space=pltpu.VMEM):
    vmem = pl.BlockSpec(memory_space=pltpu.VMEM)
    place = pl.BlockSpec(memory_space=space)
    out = jax.ShapeDtypeStruct
    if space == pltpu.HBM:
        inputs = [pltpu.with_memory_space_constraint(x, space) for x in inputs]
        out = pltpu.VMEM
    smem = pl.BlockSpec(memory_space=pltpu.SMEM)
    moved = sum(x.size * x.dtype.itemsize for x in inputs)
    return pl.pallas_call(
        kernel,
        name=name,
        in_specs=[smem if x.dtype == jnp.int32 else place for x in inputs],
        out_specs=[vmem] * len(outs),
        out_shape=[out(shape, dtype) for shape, dtype in outs],
        scratch_shapes=list(scratch),
        compiler_params=pltpu.CompilerParams(vmem_limit_bytes=VMEM_LIMIT),
        cost_estimate=pl.CostEstimate(flops=flops, bytes_accessed=moved, transcendentals=0),
    )(*inputs)


def total_of(first, others):
    total = first.astype(F32)
    for other in others:
        total = total + other.astype(F32)
    return total.astype(BF16)


def chips_of(groups, rows_out):
    return groups // 2 if rows_out % BLOCK == 0 and groups > 2 else 1


def group_sum(mine, other, size, chips):
    received = exchange(other, "group", 1, size)
    steps = range(2, size, 2)
    if chips == 1:
        piece = total_of(mine, [received])
        mine = piece = total_of(piece, [exchange(piece, "group", k, size) for k in steps])
    else:
        rows = mine.shape[1] // chips
        parts = [
            total_of(mine[:, k * rows : (k + 1) * rows], [received[:, k * rows : (k + 1) * rows]])
            for k in range(chips)
        ]
        arrived = [exchange(parts[k // 2], "group", k, size) for k in reversed(steps)]
        piece = total_of(parts[0], arrived)
        mine = jnp.concatenate(
            [piece] + [exchange(piece, "group", k, size) for k in steps], axis=1
        )
    return piece, mine, exchange(mine, "group", 1, size)


def member_sum(values, size):
    if not is_power_of_two(size):
        return lax.psum(values, "member")
    rows = values.shape[1] // 2
    low, high = values[:, :rows], values[:, rows:]
    steps = [1 << i for i in range(size.bit_length() - 1)]
    for first, second in zip(steps, reversed(steps)):
        other_low = exchange(low, "member", first, size)
        other_high = exchange(high, "member", second, size)
        low, high = total_of(low, [other_low]), total_of(high, [other_high])
    return jnp.concatenate([low, high], axis=1)


def split(values, rows):
    return values[:, :rows], values[:, rows:]


def scatter_sum(pieces, size):
    rows = pieces[0][0].shape[1]
    if size != 4:
        arrived = [
            split(exchange(jnp.concatenate(pair, axis=1), "member", k, size), rows)
            for k, pair in enumerate(pieces, start=1)
        ]
        return [low for low, _ in arrived], [high for _, high in arrived]
    (low1, high1), (low2, high2), (low3, high3) = pieces
    relay1 = exchange(low3, "member", 1, size)
    relay2 = exchange(high3, "member", 2, size)
    first1 = exchange(low1, "member", 1, size)
    first2 = exchange(high2, "member", 2, size)
    last2 = exchange(total_of(low2, [relay1]), "member", 2, size)
    last1 = exchange(total_of(high1, [relay2]), "member", 1, size)
    return [first1, last2], [first2, last1]


def gather(low, high, size):
    rows = low.shape[1]
    if size != 4:
        values = jnp.concatenate([low, high], axis=1)
        return [(low, high)] + [
            split(exchange(values, "member", k, size), rows) for k in range(1, size)
        ]
    high1 = exchange(high, "member", 1, size)
    low2 = exchange(low, "member", 2, size)
    low1 = exchange(low, "member", 1, size)
    high2 = exchange(high, "member", 2, size)
    low3 = exchange(low2, "member", 1, size)
    high3 = exchange(high1, "member", 2, size)
    return [(low, high), (low1, high1), (low2, high2), (low3, high3)]


def make_on_device(groups, members):
    steps = range(1, members)

    def on_device(
        rhs,
        leaf_pivot_inverse,
        leaf_border_block,
        leaf_map,
        mid_inverse,
        mid_border,
        root_map,
        root_inverse,
    ):
        columns = rhs.shape[3]
        leaf_pivots = rhs.shape[2]
        leaf_rows = leaf_border_block.shape[2]
        own_pivots, pivots = mid_inverse.shape[1:]
        border_rows = mid_border.shape[1]
        own_border = border_rows // members
        row_count, share_rows = root_inverse.shape
        half = share_rows // 2
        rows_out = share_rows // groups

        def flat(rows, dtype=BF16):
            return ((columns, rows), dtype)

        def spread_over_members(values):
            return [values] + [exchange(values, "member", k, members) for k in steps]

        leaf_forward, leaf_factor, leaf_edge = call(
            leaf_forward_kernel,
            "leaf_forward",
            [rhs, leaf_pivot_inverse, leaf_border_block],
            [
                flat(leaf_pivots),
                (leaf_pivot_inverse.shape[2:], BF16),
                (leaf_border_block.shape[2:], BF16),
            ],
            [
                pltpu.VMEM((leaf_pivots, columns), BF16),
                pltpu.SemaphoreType.DMA((2 + len(chunks_of(leaf_pivots)),)),
            ],
            flops=2 * columns * leaf_pivots * leaf_pivots,
            space=pltpu.HBM,
        )
        (leaf_out,) = call(
            leaf_out_kernel,
            "leaf_out",
            [leaf_forward, leaf_edge],
            [flat(leaf_rows)],
            flops=PREFETCH_FLOPS,
        )
        terms = spread_over_members(leaf_out)
        mid_forward = []
        groups_of_terms = [[0]] + [[k] for k in reversed(steps)] if members <= 4 else [[0], steps]
        for i, which in enumerate(groups_of_terms):
            last = which is groups_of_terms[-1]
            mid_forward = call(
                functools.partial(mid_forward_kernel, members, which),
                f"mid_forward_{i}",
                [leaf_map, mid_inverse, *(terms[k] for k in which), *mid_forward],
                [flat(own_pivots, BF16 if last else F32)],
                [pltpu.VMEM((columns, own_pivots), F32)],
                flops=2 * columns * own_pivots * leaf_rows * len(which),
            )
        (mid_forward,) = mid_forward
        half_border = own_border // 2
        pieces = {
            k: call(
                functools.partial(mid_piece_kernel, members, k),
                f"mid_piece_{k}",
                [mid_border, mid_forward],
                [flat(half_border), flat(half_border)],
                flops=2 * columns * own_pivots * own_border,
            )
            for k in reversed(steps)
        }
        lows, highs = scatter_sum([pieces[k] for k in steps], members)
        (own_update,) = call(
            functools.partial(own_update_kernel, members, pivots // BLOCK),
            "own_update",
            [leaf_map, mid_border, mid_forward, *terms],
            [flat(own_border, F32)],
            flops=2 * columns * own_pivots * own_border,
        )
        chips = chips_of(groups, rows_out)
        whole_share = pltpu.VMEM((columns, share_rows), BF16)
        mine, other = call(
            functools.partial(root_term_kernel, chips, groups, len(lows)),
            "root_term",
            [root_map, own_update, *lows, *highs],
            [flat(half), flat(half)],
            [whole_share],
        )
        _, mine, other = group_sum(mine, other, groups, chips)
        root_flops = columns * row_count * share_rows
        (root_own,) = call(
            functools.partial(root_own_kernel, chips, groups),
            "root_own",
            [mine, root_inverse],
            [flat(row_count, F32)],
            flops=root_flops,
        )
        (root_part,) = call(
            functools.partial(root_forward_kernel, chips, groups),
            "root_forward",
            [root_own, other, root_inverse],
            [flat(row_count)],
            flops=root_flops,
        )
        root_forward = member_sum(root_part, members)
        other, mine = (
            call(
                functools.partial(root_back_kernel, chips, groups, own),
                "root_back_own" if own else "root_back_other",
                [root_inverse, root_forward],
                [flat(half)],
                flops=root_flops,
            )[0]
            for own in (False, True)
        )
        piece, mine, other = group_sum(mine, other, groups, chips)
        own_values = call(
            functools.partial(root_pick_kernel, chips, groups),
            "root_pick",
            [root_map, mine, other],
            [flat(half_border), flat(half_border)],
            [whole_share],
        )
        shape = [((1, rows_out, columns), BF16)]
        if chips > 1:
            (root_out,) = call(root_out_kernel, "root_out", [piece], shape)
        else:
            (root_out,) = call(
                root_slice_kernel,
                "root_slice",
                [mine, other],
                shape,
                [whole_share, pltpu.VMEM((BLOCK, columns), F32)],
            )
        values = gather(*own_values, members)
        if members == 4:
            waves = [[(0, 0), (0, 1), (1, 1), (2, 0)], [(1, 0), (2, 1)], [(3, 0), (3, 1)]]
        else:
            waves = [[(0, 0), (0, 1)], [(k, h) for k in steps for h in range(2)]]
        back = mid_forward
        for i, which in enumerate(waves[:-1]):
            (back,) = call(
                functools.partial(mid_early_kernel, members, which),
                f"mid_early_{i}",
                [mid_border, back] + [values[k][h] for k, h in which],
                [flat(own_pivots, F32)],
                flops=2 * columns * own_pivots * half_border * len(which),
            )
        part, *last_pair = call(
            functools.partial(mid_back_kernel, members, waves[-1]),
            "mid_back",
            [leaf_map, mid_inverse, mid_border, back] + [values[k][h] for k, h in waves[-1]],
            [flat(pivots), flat(leaf_rows), flat(own_pivots)],
            flops=2 * columns * own_pivots * (pivots + half_border * len(waves[-1])),
        )
        pairs = [
            call(
                functools.partial(mid_share_kernel, members, k),
                f"mid_share_{k}",
                [leaf_map, part],
                [flat(leaf_rows), flat(own_pivots)],
            )
            for k in steps[:-1]
        ]
        picked, pieces = scatter_sum([*pairs, last_pair], members)
        base, own_piece = call(
            functools.partial(pick_kernel, members),
            "pick",
            [leaf_map, part] + [half for pair in values for half in pair],
            [flat(leaf_rows), flat(own_pivots)],
        )
        (leaf_values,) = call(
            leaf_back_kernel,
            "leaf_back",
            [leaf_factor, leaf_edge, leaf_forward, base, *picked],
            [((1, 1, leaf_pivots, columns), BF16)],
            flops=2 * columns * leaf_pivots * (leaf_pivots + leaf_rows),
        )
        (mid_out,) = call(
            mid_out_kernel, "mid_out", [own_piece, *pieces], [((1, own_pivots, columns), BF16)]
        )
        return leaf_values, mid_out, root_out

    return on_device


def solution(mesh):
    in_specs = (
        P("group", "member", None, None),
        P("group", "member", None, None),
        P("group", "member", None, None),
        P("group", None, None),
        P("group", "member", None),
        P("group", None, "member"),
        P("group", "member", None),
        P("group", "member"),
    )
    out_specs = (
        P("group", "member", None, None),
        P("group", "member", None),
        P("member", "group", None),
    )
    on_device = make_on_device(mesh.shape["group"], mesh.shape["member"])
    return jax.shard_map(
        on_device, mesh=mesh, in_specs=in_specs, out_specs=out_specs, check_vma=False
    )
```

```python
import functools

import jax
import jax.numpy as jnp
from jax import lax
from jax.experimental import pallas as pl
from jax.experimental.pallas import tpu as pltpu
from jax.sharding import PartitionSpec as P

BLOCK = 128
VMEM_LIMIT = 20 * 1024 * 1024
PREFETCH_FLOPS = 2 * 10**10
SHARE_FLOPS = 2 * 10**8
F32 = jnp.float32
BF16 = jnp.bfloat16


def is_power_of_two(size):
    return size & (size - 1) == 0


def partner(index, step, size):
    return index ^ step if is_power_of_two(size) else (index + step) % size


def source(index, step, size):
    return index ^ step if is_power_of_two(size) else (index - step) % size


def exchange(values, axis, step, size):
    return lax.ppermute(values, axis, [(i, partner(i, step, size)) for i in range(size)])


def times_transpose(values, matrix):
    return lax.dot_general(values, matrix, (((1,), (1,)), ((), ())), preferred_element_type=F32)


def times(values, matrix):
    return jnp.dot(values, matrix, preferred_element_type=F32)


def traced_source(index, step, size):
    if is_power_of_two(size):
        return lax.bitwise_xor(index, jnp.int32(step))
    return lax.rem(index - step + size, jnp.int32(size))


def traced_partner(index, step, size):
    if is_power_of_two(size):
        return lax.bitwise_xor(index, jnp.int32(step))
    return lax.rem(index + step, jnp.int32(size))


def at_block(index):
    return pl.ds(pl.multiple_of(index * BLOCK, BLOCK), BLOCK)


def at_part(index, size):
    return pl.ds(pl.multiple_of(index * size, BLOCK), size)


def static_block(index):
    return pl.ds(index * BLOCK, BLOCK)


def chunks_of(size):
    rows = 2 * BLOCK if size % (2 * BLOCK) == 0 else size
    return [(first, rows) for first in range(0, size, rows)]


def leaf_forward_kernel(
    rhs_hbm, factor_hbm, edge_hbm, forward_ref, factor_ref, edge_ref, rhs_ref, sems
):
    chunks = chunks_of(factor_ref.shape[0])
    copies = [pltpu.make_async_copy(rhs_hbm.at[0, 0], rhs_ref, sems.at[0])]
    for i, (first, rows) in enumerate(chunks, start=1):
        part = (pl.ds(first, rows), pl.ds(0, first + rows))
        copies.append(
            pltpu.make_async_copy(factor_hbm.at[0, 0, *part], factor_ref.at[*part], sems.at[i])
        )
    edge_copy = pltpu.make_async_copy(edge_hbm.at[0, 0], edge_ref, sems.at[1 + len(chunks)])
    for copy in copies:
        copy.start()
    edge_copy.start()
    copies[0].wait()
    source_rows = rhs_ref[...].T
    for copy, (first, rows) in zip(copies[1:], chunks):
        copy.wait()
        factor = factor_ref[pl.ds(first, rows), pl.ds(0, first + rows)]
        forward = times_transpose(source_rows[:, : first + rows], factor)
        forward_ref[:, pl.ds(first, rows)] = forward.astype(BF16)
    edge_copy.wait()


def leaf_out_kernel(forward_ref, edge_ref, out_ref):
    out_ref[...] = (-times_transpose(forward_ref[...], edge_ref[...])).astype(BF16)


def border_piece(border_ref, owner, rows):
    return border_ref[0, pl.ds(pl.multiple_of(owner * rows, BLOCK), rows), :]


def mid_forward_kernel(members, which, map_ref, inverse_ref, *refs):
    forward_ref = refs[-1]
    terms = refs[: len(which)]
    before = refs[len(which) : -1]
    pivot_blocks = inverse_ref.shape[2] // BLOCK
    member = lax.axis_index("member")
    total = before[0][...] if before else None
    for k, term in zip(which, terms):
        owner = traced_source(member, k, members)
        blocks = range(term.shape[1] // BLOCK)
        for first in blocks[::2]:
            values, columns = [], []
            for j in blocks[first : first + 2]:
                target = map_ref[0, owner, j]
                block = term[:, static_block(j)]
                values.append(jnp.where(target < pivot_blocks, block, jnp.zeros_like(block)))
                columns.append(inverse_ref[0, :, at_block(lax.min(target, pivot_blocks - 1))])
            part = times_transpose(
                jnp.concatenate(values, axis=1), jnp.concatenate(columns, axis=1)
            )
            total = part if total is None else total + part
    forward_ref[...] = total.astype(forward_ref.dtype)


def mid_piece_kernel(members, step, border_ref, forward_ref, low_ref, high_ref):
    owner = traced_partner(lax.axis_index("member"), step, members)
    rows = low_ref.shape[1]
    for half, ref in enumerate((low_ref, high_ref)):
        piece = border_piece(border_ref, 2 * owner + half, rows)
        ref[...] = (-times_transpose(forward_ref[...], piece)).astype(BF16)


def own_update_kernel(members, pivot_blocks, *refs):
    map_ref, border_ref, forward_ref = refs[:3]
    terms = refs[3 : 3 + members]
    update_ref = refs[-1]
    member = lax.axis_index("member")
    rows = update_ref.shape[1]
    piece = border_ref[0, pl.ds(pl.multiple_of(member * rows, BLOCK), rows), :]
    update_ref[...] = -times_transpose(forward_ref[...], piece)
    first = pivot_blocks + member * (rows // BLOCK)
    for k, term in enumerate(terms):
        owner = traced_source(member, k, members)
        for j in range(term.shape[1] // BLOCK):
            target = map_ref[0, owner, j] - first

            @pl.when((target >= 0) & (target < rows // BLOCK))
            def _():
                update_ref[:, at_block(target)] += term[:, static_block(j)].astype(F32)


def pieces_of(core, chips, groups, half):
    if chips == 1:
        return [core * half]
    chip = lax.axis_index("group") // 2
    rows = half // chips
    return [(2 * traced_partner(chip, k, chips) + core) * rows for k in range(chips)]


def take_half(ref, spread, core, chips, groups):
    half = ref.shape[1]
    rows = half // chips
    for k, first in enumerate(pieces_of(core, chips, groups, half)):
        ref[:, pl.ds(k * rows, rows)] = spread[:, pl.ds(pl.multiple_of(first, BLOCK), rows)]


def root_term_kernel(chips, groups, lows, *refs):
    map_ref, own_ref = refs[:2]
    arrived = (refs[2 : 2 + lows], refs[2 + lows : -3])
    mine_ref, other_ref, spread = refs[-3:]
    core = lax.axis_index("group") & 1
    spread[...] = jnp.zeros_like(spread)
    half_blocks = own_ref.shape[1] // (2 * BLOCK)
    for i in range(2 * half_blocks):
        total = own_ref[:, static_block(i)]
        for term in arrived[i // half_blocks]:
            total = total + term[:, static_block(i % half_blocks)].astype(F32)
        spread[:, at_block(map_ref[0, 0, i])] = total.astype(BF16)
    take_half(other_ref, spread, 1 - core, chips, groups)
    take_half(mine_ref, spread, core, chips, groups)


def join(joined, mine_ref, other_ref, chips, groups):
    core = lax.axis_index("group") & 1
    half = mine_ref.shape[1]
    rows = half // chips
    for ref, owner in ((mine_ref, core), (other_ref, 1 - core)):
        for k, first in enumerate(pieces_of(owner, chips, groups, half)):
            joined[:, pl.ds(pl.multiple_of(first, BLOCK), rows)] = ref[:, pl.ds(k * rows, rows)]


def root_half(chips, groups, owner, half_ref, inverse_ref, lines):
    half = half_ref.shape[1]
    rows = half // chips
    total = None
    for k, first in enumerate(pieces_of(owner, chips, groups, half)):
        columns = inverse_ref[lines, pl.ds(pl.multiple_of(first, BLOCK), rows)]
        part = times_transpose(half_ref[:, pl.ds(k * rows, rows)], columns)
        total = part if total is None else total + part
    return total


def root_own_kernel(chips, groups, mine_ref, inverse_ref, *outs):
    core = lax.axis_index("group") & 1
    rows = outs[0].shape[1]
    for i, out_ref in enumerate(outs):
        lines = pl.ds(i * rows, rows)
        out_ref[...] = root_half(chips, groups, core, mine_ref, inverse_ref, lines)


def root_forward_kernel(chips, groups, part, own_ref, other_ref, inverse_ref, out_ref):
    core = lax.axis_index("group") & 1
    rows = out_ref.shape[1]
    lines = pl.ds(part * rows, rows)
    product = root_half(chips, groups, 1 - core, other_ref, inverse_ref, lines)
    out_ref[...] = (own_ref[...] + product).astype(BF16)


def root_back_kernel(chips, groups, own, part, inverse_ref, forward_ref, *refs):
    half_ref = refs[-1]
    core = lax.axis_index("group") & 1
    half = half_ref.shape[1]
    rows = half // chips
    forward = forward_ref[...]
    lines = pl.ds(part * forward.shape[1], forward.shape[1])
    for k, first in enumerate(pieces_of(core if own else 1 - core, chips, groups, half)):
        place = pl.ds(k * rows, rows)
        columns = inverse_ref[lines, pl.ds(pl.multiple_of(first, BLOCK), rows)]
        total = times(forward, columns)
        for before in refs[:-1]:
            total = total + before[:, place]
        half_ref[:, place] = total.astype(half_ref.dtype)


def root_pick_kernel(chips, groups, map_ref, mine_ref, other_ref, low_ref, high_ref, joined):
    join(joined, mine_ref, other_ref, chips, groups)
    blocks = low_ref.shape[1] // BLOCK
    for i in range(2 * blocks):
        ref = (low_ref, high_ref)[i // blocks]
        ref[:, static_block(i % blocks)] = joined[:, at_block(map_ref[0, 0, i])]


def root_out_kernel(total_ref, out_ref):
    out_ref[0] = total_ref[...].astype(F32).T.astype(BF16)


def root_slice_kernel(mine_ref, other_ref, out_ref, joined, turned):
    join(joined, mine_ref, other_ref, 1, 0)
    rows_out = out_ref.shape[1]
    first = lax.axis_index("group") * rows_out
    turned[...] = joined[:, at_block(first // BLOCK)].astype(F32).T
    begin = pl.multiple_of(lax.rem(first, jnp.int32(BLOCK)), rows_out)
    out_ref[0] = turned[pl.ds(begin, rows_out), :].astype(BF16)


def border_product(members, values, which, border_ref):
    member = lax.axis_index("member")
    total = None
    for (step, half), ref in zip(which, values):
        owner = traced_source(member, step, members)
        piece = border_piece(border_ref, 2 * owner + half, ref.shape[1])
        part = times(ref[...], piece)
        total = part if total is None else total + part
    return total


def mid_early_kernel(members, which, border_ref, back_ref, *refs):
    product = border_product(members, refs[:-1], which, border_ref)
    refs[-1][...] = back_ref[...].astype(F32) - product


def ask(map_ref, owner, part_ref, out_ref):
    pivot_blocks = part_ref.shape[1] // BLOCK
    for j in range(out_ref.shape[1] // BLOCK):
        target = map_ref[0, owner, j]
        block = part_ref[:, at_block(lax.min(target, pivot_blocks - 1))]
        out_ref[:, static_block(j)] = jnp.where(
            target < pivot_blocks, block, jnp.zeros_like(block)
        )


def mid_back_kernel(members, late, map_ref, inverse_ref, border_ref, back_ref, *refs):
    values = refs[:-3]
    part_ref, asked_ref, piece_ref = refs[-3:]
    back = back_ref[...] - border_product(members, values, late, border_ref)
    part_ref[...] = times(back.astype(BF16), inverse_ref[0]).astype(BF16)
    owner = traced_partner(lax.axis_index("member"), members - 1, members)
    ask(map_ref, owner, part_ref, asked_ref)
    piece_ref[...] = part_ref[:, at_part(owner, piece_ref.shape[1])]


def mid_share_kernel(members, step, map_ref, part_ref, asked_ref, piece_ref):
    owner = traced_partner(lax.axis_index("member"), step, members)
    ask(map_ref, owner, part_ref, asked_ref)
    piece_ref[...] = part_ref[:, at_part(owner, piece_ref.shape[1])]


def pick_kernel(members, map_ref, part_ref, *refs):
    values = refs[:-2]
    base_ref, own_ref = refs[-2:]
    member = lax.axis_index("member")
    pivot_blocks = part_ref.shape[1] // BLOCK
    rows = values[0].shape[1]
    for j in range(base_ref.shape[1] // BLOCK):
        target = map_ref[0, member, j]

        @pl.when(target < pivot_blocks)
        def _():
            base_ref[:, static_block(j)] = part_ref[:, at_block(target)]

        border = target - pivot_blocks
        for k, values_ref in enumerate(values):
            owner = traced_source(member, k // 2, members)
            inner = border - (2 * owner + k % 2) * (rows // BLOCK)

            @pl.when((border >= 0) & (inner >= 0) & (inner < rows // BLOCK))
            def _():
                base_ref[:, static_block(j)] = values_ref[:, at_block(inner)]

    own_ref[...] = part_ref[:, at_part(member, own_ref.shape[1])]


def leaf_back_kernel(*refs):
    factor_ref, edge_ref, forward_ref = refs[:3]
    terms = refs[3:-1]
    out_ref = refs[-1]
    picked = terms[0][...].astype(F32)
    for term in terms[1:]:
        picked = picked + term[...].astype(F32)
    back = forward_ref[...].astype(F32) - times(picked.astype(BF16), edge_ref[...])
    back = back.astype(BF16)
    chunks = chunks_of(factor_ref.shape[0])
    for first, rows in chunks:
        total = None
        for lower, size in chunks:
            if lower >= first:
                factor = factor_ref[pl.ds(lower, size), pl.ds(first, rows)]
                part = times(back[:, lower : lower + size], factor)
                total = part if total is None else total + part
        out_ref[0, 0, pl.ds(first, rows), :] = total.T.astype(BF16)


def mid_out_kernel(*refs):
    total = refs[0][...].astype(F32)
    for term in refs[1:-1]:
        total = total + term[...].astype(F32)
    refs[-1][0] = total.T.astype(BF16)


def call(kernel, name, inputs, outs, scratch=(), flops=0, space=pltpu.VMEM):
    vmem = pl.BlockSpec(memory_space=pltpu.VMEM)
    place = pl.BlockSpec(memory_space=space)
    out = jax.ShapeDtypeStruct
    if space == pltpu.HBM:
        inputs = [pltpu.with_memory_space_constraint(x, space) for x in inputs]
        out = pltpu.VMEM
    smem = pl.BlockSpec(memory_space=pltpu.SMEM)
    moved = sum(x.size * x.dtype.itemsize for x in inputs)
    return pl.pallas_call(
        kernel,
        name=name,
        in_specs=[smem if x.dtype == jnp.int32 else place for x in inputs],
        out_specs=[vmem] * len(outs),
        out_shape=[out(shape, dtype) for shape, dtype in outs],
        scratch_shapes=list(scratch),
        compiler_params=pltpu.CompilerParams(vmem_limit_bytes=VMEM_LIMIT),
        cost_estimate=pl.CostEstimate(flops=flops, bytes_accessed=moved, transcendentals=0),
    )(*inputs)


def total_of(first, others):
    total = first.astype(F32)
    for other in others:
        total = total + other.astype(F32)
    return total.astype(BF16)


def chips_of(groups, rows_out):
    return groups // 2 if rows_out % BLOCK == 0 and groups > 2 else 1


def group_sum(mine, other, size, chips):
    received = exchange(other, "group", 1, size)
    steps = range(2, size, 2)
    if chips == 1:
        piece = total_of(mine, [received])
        mine = piece = total_of(piece, [exchange(piece, "group", k, size) for k in steps])
    else:
        rows = mine.shape[1] // chips
        parts = [
            total_of(mine[:, k * rows : (k + 1) * rows], [received[:, k * rows : (k + 1) * rows]])
            for k in range(chips)
        ]
        arrived = [exchange(parts[k // 2], "group", k, size) for k in reversed(steps)]
        piece = total_of(parts[0], arrived)
        mine = jnp.concatenate(
            [piece] + [exchange(piece, "group", k, size) for k in steps], axis=1
        )
    return piece, mine, exchange(mine, "group", 1, size)


def member_sum(low, high, size):
    if not is_power_of_two(size):
        return lax.psum(low, "member"), lax.psum(high, "member")
    steps = [1 << i for i in range(size.bit_length() - 1)]
    for first, second in zip(steps, reversed(steps)):
        other_low = exchange(low, "member", first, size)
        other_high = exchange(high, "member", second, size)
        low, high = total_of(low, [other_low]), total_of(high, [other_high])
    return low, high


def split(values, rows):
    return values[:, :rows], values[:, rows:]


def scatter_sum(pieces, size):
    rows = pieces[0][0].shape[1]
    if size != 4:
        arrived = [
            split(exchange(jnp.concatenate(pair, axis=1), "member", k, size), rows)
            for k, pair in enumerate(pieces, start=1)
        ]
        return [low for low, _ in arrived], [high for _, high in arrived]
    (low1, high1), (low2, high2), (low3, high3) = pieces
    relay1 = exchange(low3, "member", 1, size)
    relay2 = exchange(high3, "member", 2, size)
    first1 = exchange(low1, "member", 1, size)
    first2 = exchange(high2, "member", 2, size)
    last2 = exchange(total_of(low2, [relay1]), "member", 2, size)
    last1 = exchange(total_of(high1, [relay2]), "member", 1, size)
    return [first1, last2], [first2, last1]


def gather(low, high, size):
    rows = low.shape[1]
    if size != 4:
        values = jnp.concatenate([low, high], axis=1)
        return [(low, high)] + [
            split(exchange(values, "member", k, size), rows) for k in range(1, size)
        ]
    high1 = exchange(high, "member", 1, size)
    low2 = exchange(low, "member", 2, size)
    low1 = exchange(low, "member", 1, size)
    high2 = exchange(high, "member", 2, size)
    low3 = exchange(low2, "member", 1, size)
    high3 = exchange(high1, "member", 2, size)
    return [(low, high), (low1, high1), (low2, high2), (low3, high3)]


def make_on_device(groups, members):
    steps = range(1, members)

    def on_device(
        rhs,
        leaf_pivot_inverse,
        leaf_border_block,
        leaf_map,
        mid_inverse,
        mid_border,
        root_map,
        root_inverse,
    ):
        columns = rhs.shape[3]
        leaf_pivots = rhs.shape[2]
        leaf_rows = leaf_border_block.shape[2]
        own_pivots, pivots = mid_inverse.shape[1:]
        border_rows = mid_border.shape[1]
        own_border = border_rows // members
        row_count, share_rows = root_inverse.shape
        half = share_rows // 2
        rows_out = share_rows // groups

        def flat(rows, dtype=BF16):
            return ((columns, rows), dtype)

        def spread_over_members(values):
            return [values] + [exchange(values, "member", k, members) for k in steps]

        leaf_forward, leaf_factor, leaf_edge = call(
            leaf_forward_kernel,
            "leaf_forward",
            [rhs, leaf_pivot_inverse, leaf_border_block],
            [
                flat(leaf_pivots),
                (leaf_pivot_inverse.shape[2:], BF16),
                (leaf_border_block.shape[2:], BF16),
            ],
            [
                pltpu.VMEM((leaf_pivots, columns), BF16),
                pltpu.SemaphoreType.DMA((2 + len(chunks_of(leaf_pivots)),)),
            ],
            flops=2 * columns * leaf_pivots * leaf_pivots,
            space=pltpu.HBM,
        )
        (leaf_out,) = call(
            leaf_out_kernel,
            "leaf_out",
            [leaf_forward, leaf_edge],
            [flat(leaf_rows)],
            flops=PREFETCH_FLOPS,
        )
        terms = spread_over_members(leaf_out)
        mid_forward = []
        groups_of_terms = [[0], list(steps)]
        if members == 4:
            groups_of_terms = [[0], [3], [2, 1]]
        for i, which in enumerate(groups_of_terms):
            last = which is groups_of_terms[-1]
            mid_forward = call(
                functools.partial(mid_forward_kernel, members, which),
                f"mid_forward_{i}",
                [leaf_map, mid_inverse, *(terms[k] for k in which), *mid_forward],
                [flat(own_pivots, BF16 if last else F32)],
                flops=2 * columns * own_pivots * leaf_rows * len(which),
            )
        (mid_forward,) = mid_forward
        half_border = own_border // 2
        pieces = {
            k: call(
                functools.partial(mid_piece_kernel, members, k),
                f"mid_piece_{k}",
                [mid_border, mid_forward],
                [flat(half_border), flat(half_border)],
                flops=2 * columns * own_pivots * own_border,
            )
            for k in reversed(steps)
        }
        lows, highs = scatter_sum([pieces[k] for k in steps], members)
        (own_update,) = call(
            functools.partial(own_update_kernel, members, pivots // BLOCK),
            "own_update",
            [leaf_map, mid_border, mid_forward, *terms],
            [flat(own_border, F32)],
            flops=2 * columns * own_pivots * own_border,
        )
        chips = chips_of(groups, rows_out)
        whole_share = pltpu.VMEM((columns, share_rows), BF16)
        mine, other = call(
            functools.partial(root_term_kernel, chips, groups, len(lows)),
            "root_term",
            [root_map, own_update, *lows, *highs],
            [flat(half), flat(half)],
            [whole_share],
        )
        _, mine, other = group_sum(mine, other, groups, chips)
        root_flops = columns * row_count * share_rows
        half_count = row_count // 2
        root_own = call(
            functools.partial(root_own_kernel, chips, groups),
            "root_own",
            [mine, root_inverse],
            [flat(half_count, F32), flat(half_count, F32)],
            flops=root_flops,
        )
        root_parts = [
            call(
                functools.partial(root_forward_kernel, chips, groups, part),
                f"root_forward_{part}",
                [own, other, root_inverse],
                [flat(half_count)],
                flops=root_flops // 2,
            )[0]
            for part, own in enumerate(root_own)
        ]
        root_forward = member_sum(*root_parts, members)
        halves = {}
        for own in (False, True):
            before = []
            for part, forward in enumerate(root_forward):
                before = call(
                    functools.partial(root_back_kernel, chips, groups, own, part),
                    f"root_back_{own}_{part}",
                    [root_inverse, forward, *before],
                    [flat(half, BF16 if part else F32)],
                    flops=root_flops // 2,
                )
            (halves[own],) = before
        mine, other = halves[True], halves[False]
        piece, mine, other = group_sum(mine, other, groups, chips)
        own_values = call(
            functools.partial(root_pick_kernel, chips, groups),
            "root_pick",
            [root_map, mine, other],
            [flat(half_border), flat(half_border)],
            [whole_share],
        )
        shape = [((1, rows_out, columns), BF16)]
        if chips > 1:
            (root_out,) = call(root_out_kernel, "root_out", [piece], shape)
        else:
            (root_out,) = call(
                root_slice_kernel,
                "root_slice",
                [mine, other],
                shape,
                [whole_share, pltpu.VMEM((BLOCK, columns), F32)],
            )
        values = gather(*own_values, members)
        if members == 4:
            waves = [[(0, 0), (0, 1), (1, 1), (2, 0)], [(1, 0), (2, 1)], [(3, 0), (3, 1)]]
        else:
            waves = [[(0, 0), (0, 1)], [(k, h) for k in steps for h in range(2)]]
        back = mid_forward
        for i, which in enumerate(waves[:-1]):
            (back,) = call(
                functools.partial(mid_early_kernel, members, which),
                f"mid_early_{i}",
                [mid_border, back] + [values[k][h] for k, h in which],
                [flat(own_pivots, F32)],
                flops=2 * columns * own_pivots * half_border * len(which),
            )
        part, *last_pair = call(
            functools.partial(mid_back_kernel, members, waves[-1]),
            "mid_back",
            [leaf_map, mid_inverse, mid_border, back] + [values[k][h] for k, h in waves[-1]],
            [flat(pivots), flat(leaf_rows), flat(own_pivots)],
            flops=2 * columns * own_pivots * (pivots + half_border * len(waves[-1])),
        )
        pairs = [
            call(
                functools.partial(mid_share_kernel, members, k),
                f"mid_share_{k}",
                [leaf_map, part],
                [flat(leaf_rows), flat(own_pivots)],
                flops=SHARE_FLOPS,
            )
            for k in steps[:-1]
        ]
        picked, pieces = scatter_sum([*pairs, last_pair], members)
        base, own_piece = call(
            functools.partial(pick_kernel, members),
            "pick",
            [leaf_map, part] + [half for pair in values for half in pair],
            [flat(leaf_rows), flat(own_pivots)],
            flops=SHARE_FLOPS,
        )
        (leaf_values,) = call(
            leaf_back_kernel,
            "leaf_back",
            [leaf_factor, leaf_edge, leaf_forward, base, *picked],
            [((1, 1, leaf_pivots, columns), BF16)],
            flops=2 * columns * leaf_pivots * (leaf_pivots + leaf_rows),
        )
        (mid_out,) = call(
            mid_out_kernel, "mid_out", [own_piece, *pieces], [((1, own_pivots, columns), BF16)]
        )
        return leaf_values, mid_out, root_out

    return on_device


def solution(mesh):
    in_specs = (
        P("group", "member", None, None),
        P("group", "member", None, None),
        P("group", "member", None, None),
        P("group", None, None),
        P("group", "member", None),
        P("group", None, "member"),
        P("group", "member", None),
        P("group", "member"),
    )
    out_specs = (
        P("group", "member", None, None),
        P("group", "member", None),
        P("member", "group", None),
    )
    on_device = make_on_device(mesh.shape["group"], mesh.shape["member"])
    return jax.shard_map(
        on_device, mesh=mesh, in_specs=in_specs, out_specs=out_specs, check_vma=False
    )
```

```python
import functools

import jax
import jax.numpy as jnp
from jax import lax
from jax.experimental import pallas as pl
from jax.experimental.pallas import tpu as pltpu
from jax.sharding import PartitionSpec as P

BLOCK = 128
VMEM_LIMIT = 20 * 1024 * 1024
PREFETCH_FLOPS = 2 * 10**10
SHARE_FLOPS = 2 * 10**8
F32 = jnp.float32
BF16 = jnp.bfloat16


def is_power_of_two(size):
    return size & (size - 1) == 0


def partner(index, step, size):
    return index ^ step if is_power_of_two(size) else (index + step) % size


def source(index, step, size):
    return index ^ step if is_power_of_two(size) else (index - step) % size


def exchange(values, axis, step, size):
    return lax.ppermute(values, axis, [(i, partner(i, step, size)) for i in range(size)])


def times_transpose(values, matrix):
    return lax.dot_general(values, matrix, (((1,), (1,)), ((), ())), preferred_element_type=F32)


def times(values, matrix):
    return jnp.dot(values, matrix, preferred_element_type=F32)


def traced_source(index, step, size):
    if is_power_of_two(size):
        return lax.bitwise_xor(index, jnp.int32(step))
    return lax.rem(index - step + size, jnp.int32(size))


def traced_partner(index, step, size):
    if is_power_of_two(size):
        return lax.bitwise_xor(index, jnp.int32(step))
    return lax.rem(index + step, jnp.int32(size))


def at_block(index):
    return pl.ds(pl.multiple_of(index * BLOCK, BLOCK), BLOCK)


def at_part(index, size):
    return pl.ds(pl.multiple_of(index * size, BLOCK), size)


def static_block(index):
    return pl.ds(index * BLOCK, BLOCK)


def chunks_of(size):
    rows = 2 * BLOCK if size % (2 * BLOCK) == 0 else size
    return [(first, rows) for first in range(0, size, rows)]


def leaf_forward_kernel(
    rhs_hbm,
    factor_hbm,
    edge_hbm,
    leaf_map_hbm,
    root_map_hbm,
    forward_ref,
    factor_ref,
    edge_ref,
    leaf_map_ref,
    root_map_ref,
    rhs_ref,
    sems,
):
    chunks = chunks_of(factor_ref.shape[0])
    copies = [pltpu.make_async_copy(rhs_hbm.at[0, 0], rhs_ref, sems.at[0])]
    for i, (first, rows) in enumerate(chunks, start=1):
        part = (pl.ds(first, rows), pl.ds(0, first + rows))
        copies.append(
            pltpu.make_async_copy(factor_hbm.at[0, 0, *part], factor_ref.at[*part], sems.at[i])
        )
    later = [
        pltpu.make_async_copy(source_ref, target_ref, sems.at[1 + len(chunks) + i])
        for i, (source_ref, target_ref) in enumerate(
            (
                (edge_hbm.at[0, 0], edge_ref),
                (leaf_map_hbm, leaf_map_ref),
                (root_map_hbm, root_map_ref),
            )
        )
    ]
    for copy in copies + later:
        copy.start()
    copies[0].wait()
    source_rows = rhs_ref[...].T
    for copy, (first, rows) in zip(copies[1:], chunks):
        copy.wait()
        factor = factor_ref[pl.ds(first, rows), pl.ds(0, first + rows)]
        forward = times_transpose(source_rows[:, : first + rows], factor)
        forward_ref[:, pl.ds(first, rows)] = forward.astype(BF16)
    for copy in later:
        copy.wait()


def leaf_out_kernel(forward_ref, edge_ref, out_ref):
    out_ref[...] = (-times_transpose(forward_ref[...], edge_ref[...])).astype(BF16)


def border_piece(border_ref, owner, rows):
    return border_ref[0, pl.ds(pl.multiple_of(owner * rows, BLOCK), rows), :]


def mid_forward_kernel(members, which, map_ref, inverse_ref, *refs):
    forward_ref = refs[-1]
    terms = refs[: len(which)]
    before = refs[len(which) : -1]
    pivot_blocks = inverse_ref.shape[2] // BLOCK
    member = lax.axis_index("member")
    total = before[0][...] if before else None
    for k, term in zip(which, terms):
        owner = traced_source(member, k, members)
        blocks = range(term.shape[1] // BLOCK)
        for first in blocks[::2]:
            values, columns = [], []
            for j in blocks[first : first + 2]:
                target = map_ref[0, owner, j]
                block = term[:, static_block(j)]
                values.append(jnp.where(target < pivot_blocks, block, jnp.zeros_like(block)))
                columns.append(inverse_ref[0, :, at_block(lax.min(target, pivot_blocks - 1))])
            part = times_transpose(
                jnp.concatenate(values, axis=1), jnp.concatenate(columns, axis=1)
            )
            total = part if total is None else total + part
    forward_ref[...] = total.astype(forward_ref.dtype)


def mid_piece_kernel(members, step, border_ref, forward_ref, low_ref, high_ref):
    owner = traced_partner(lax.axis_index("member"), step, members)
    rows = low_ref.shape[1]
    for half, ref in enumerate((low_ref, high_ref)):
        piece = border_piece(border_ref, 2 * owner + half, rows)
        ref[...] = (-times_transpose(forward_ref[...], piece)).astype(BF16)


def own_update_kernel(members, pivot_blocks, *refs):
    map_ref, border_ref, forward_ref = refs[:3]
    terms = refs[3 : 3 + members]
    update_ref = refs[-1]
    member = lax.axis_index("member")
    rows = update_ref.shape[1]
    piece = border_ref[0, pl.ds(pl.multiple_of(member * rows, BLOCK), rows), :]
    update_ref[...] = -times_transpose(forward_ref[...], piece)
    first = pivot_blocks + member * (rows // BLOCK)
    for k, term in enumerate(terms):
        owner = traced_source(member, k, members)
        for j in range(term.shape[1] // BLOCK):
            target = map_ref[0, owner, j] - first

            @pl.when((target >= 0) & (target < rows // BLOCK))
            def _():
                update_ref[:, at_block(target)] += term[:, static_block(j)].astype(F32)


DISTANCES = (0, 2, 1, 3)


def is_split(chips):
    return chips == len(DISTANCES)


def stream_places(core, chips, share):
    if not is_split(chips):
        return [[core * (share // 2)]], share // 2
    chip = lax.axis_index("group") // 2
    size = share // (4 * chips)
    owners = [2 * lax.bitwise_xor(chip, jnp.int32(k)) + core for k in DISTANCES]
    return [[(2 * owner + stream) * size for owner in owners] for stream in range(2)], size


def unit_places(core, chips, share):
    streams, size = stream_places(core, chips, share)
    if not is_split(chips):
        return streams, size
    return [places[i : i + 2] for places in streams for i in (0, 2)], size


def at_places(ref, lines, places, size):
    parts = [ref[lines, pl.ds(pl.multiple_of(place, BLOCK), size)] for place in places]
    return parts[0] if len(parts) == 1 else jnp.concatenate(parts, axis=1)


def take_streams(refs, spread, core, chips):
    streams, size = stream_places(core, chips, spread.shape[1])
    for ref, places in zip(refs, streams):
        for i, place in enumerate(places):
            ref[:, pl.ds(i * size, size)] = spread[:, pl.ds(pl.multiple_of(place, BLOCK), size)]


def root_term_kernel(chips, lows, *refs):
    count = 2 if is_split(chips) else 1
    inputs, outs, spread = refs[: -1 - 2 * count], refs[-1 - 2 * count : -1], refs[-1]
    map_ref, own_ref = inputs[:2]
    arrived = (inputs[2 : 2 + lows], inputs[2 + lows :])
    core = lax.axis_index("group") & 1
    spread[...] = jnp.zeros_like(spread)
    half_blocks = own_ref.shape[1] // (2 * BLOCK)
    for i in range(2 * half_blocks):
        total = own_ref[:, static_block(i)]
        for term in arrived[i // half_blocks]:
            total = total + term[:, static_block(i % half_blocks)].astype(F32)
        spread[:, at_block(map_ref[0, 0, i])] = total.astype(BF16)
    take_streams(outs[:count], spread, 1 - core, chips)
    take_streams(outs[count:], spread, core, chips)


def join(joined, units, chips):
    core = lax.axis_index("group") & 1
    count = len(units) // 2
    for owner, refs in ((core, units[:count]), (1 - core, units[count:])):
        places_of, size = unit_places(owner, chips, joined.shape[1])
        for ref, places in zip(refs, places_of):
            for i, place in enumerate(places):
                target = pl.ds(pl.multiple_of(place, BLOCK), size)
                joined[:, target] = ref[:, pl.ds(i * size, size)]


def root_product(chips, which, units, inverse_ref, lines):
    core = lax.axis_index("group") & 1
    total = None
    for (own, number), ref in zip(which, units):
        places_of, size = unit_places(core if own else 1 - core, chips, inverse_ref.shape[1])
        columns = at_places(inverse_ref, lines, places_of[number], size)
        part = times_transpose(ref[...], columns)
        total = part if total is None else total + part
    return total


def root_early_kernel(chips, which, inverse_ref, *refs):
    units, before, outs = refs[: len(which)], refs[len(which) : -2], refs[-2:]
    rows = outs[0].shape[1]
    for part, out_ref in enumerate(outs):
        total = root_product(chips, which, units, inverse_ref, pl.ds(part * rows, rows))
        out_ref[...] = total + before[part][...] if before else total


def root_forward_kernel(chips, which, part, inverse_ref, *refs):
    units, before_ref, out_ref = refs[:-2], refs[-2], refs[-1]
    rows = out_ref.shape[1]
    total = root_product(chips, which, units, inverse_ref, pl.ds(part * rows, rows))
    out_ref[...] = (total + before_ref[...]).astype(BF16)


def root_back_kernel(chips, own, part, inverse_ref, forward_ref, *refs):
    count = 2 if is_split(chips) else 1
    before, outs = refs[:-count], refs[-count:]
    core = lax.axis_index("group") & 1
    streams, size = stream_places(core if own else 1 - core, chips, inverse_ref.shape[1])
    forward = forward_ref[...]
    lines = pl.ds(part * forward.shape[1], forward.shape[1])
    for i, (places, out_ref) in enumerate(zip(streams, outs)):
        total = times(forward, at_places(inverse_ref, lines, places, size))
        if before:
            total = total + before[i][...]
        out_ref[...] = total.astype(out_ref.dtype)


def root_pick_kernel(chips, map_ref, *refs):
    units, (low_ref, high_ref, joined) = refs[:-3], refs[-3:]
    join(joined, units, chips)
    blocks = low_ref.shape[1] // BLOCK
    for i in range(2 * blocks):
        ref = (low_ref, high_ref)[i // blocks]
        ref[:, static_block(i % blocks)] = joined[:, at_block(map_ref[0, 0, i])]


def root_out_kernel(low_ref, high_ref, out_ref):
    rows = out_ref.shape[1] // 2
    for i, ref in enumerate((low_ref, high_ref)):
        block = ref[:, pl.ds(0, rows)].astype(F32).T
        out_ref[0, pl.ds(i * rows, rows), :] = block.astype(BF16)


def root_slice_kernel(mine_ref, other_ref, out_ref, joined, turned):
    join(joined, (mine_ref, other_ref), 1)
    rows_out = out_ref.shape[1]
    first = lax.axis_index("group") * rows_out
    rows = turned.shape[0]
    turned[...] = joined[:, at_part(first // rows, rows)].astype(F32).T
    begin = pl.multiple_of(lax.rem(first, jnp.int32(rows)), min(rows_out, rows))
    out_ref[0] = turned[pl.ds(begin, rows_out), :].astype(BF16)


def border_product(members, values, which, border_ref):
    member = lax.axis_index("member")
    total = None
    for (step, half), ref in zip(which, values):
        owner = traced_source(member, step, members)
        piece = border_piece(border_ref, 2 * owner + half, ref.shape[1])
        part = times(ref[...], piece)
        total = part if total is None else total + part
    return total


def mid_early_kernel(members, which, border_ref, back_ref, *refs):
    product = border_product(members, refs[:-1], which, border_ref)
    refs[-1][...] = back_ref[...].astype(F32) - product


def ask(map_ref, owner, part_ref, out_ref):
    pivot_blocks = part_ref.shape[1] // BLOCK
    for j in range(out_ref.shape[1] // BLOCK):
        target = map_ref[0, owner, j]
        block = part_ref[:, at_block(lax.min(target, pivot_blocks - 1))]
        out_ref[:, static_block(j)] = jnp.where(
            target < pivot_blocks, block, jnp.zeros_like(block)
        )


def mid_back_kernel(members, late, map_ref, inverse_ref, border_ref, back_ref, *refs):
    values = refs[:-3]
    part_ref, asked_ref, piece_ref = refs[-3:]
    back = back_ref[...] - border_product(members, values, late, border_ref)
    part_ref[...] = times(back.astype(BF16), inverse_ref[0]).astype(BF16)
    owner = traced_partner(lax.axis_index("member"), members - 1, members)
    ask(map_ref, owner, part_ref, asked_ref)
    piece_ref[...] = part_ref[:, at_part(owner, piece_ref.shape[1])]


def mid_share_kernel(members, step, map_ref, part_ref, asked_ref, piece_ref):
    owner = traced_partner(lax.axis_index("member"), step, members)
    ask(map_ref, owner, part_ref, asked_ref)
    piece_ref[...] = part_ref[:, at_part(owner, piece_ref.shape[1])]


def pick_kernel(members, map_ref, part_ref, *refs):
    values = refs[:-2]
    base_ref, own_ref = refs[-2:]
    member = lax.axis_index("member")
    pivot_blocks = part_ref.shape[1] // BLOCK
    rows = values[0].shape[1]
    for j in range(base_ref.shape[1] // BLOCK):
        target = map_ref[0, member, j]

        @pl.when(target < pivot_blocks)
        def _():
            base_ref[:, static_block(j)] = part_ref[:, at_block(target)]

        border = target - pivot_blocks
        for k, values_ref in enumerate(values):
            owner = traced_source(member, k // 2, members)
            inner = border - (2 * owner + k % 2) * (rows // BLOCK)

            @pl.when((border >= 0) & (inner >= 0) & (inner < rows // BLOCK))
            def _():
                base_ref[:, static_block(j)] = values_ref[:, at_block(inner)]

    own_ref[...] = part_ref[:, at_part(member, own_ref.shape[1])]


def leaf_back_kernel(*refs):
    factor_ref, edge_ref, forward_ref = refs[:3]
    terms = refs[3:-1]
    out_ref = refs[-1]
    picked = terms[0][...].astype(F32)
    for term in terms[1:]:
        picked = picked + term[...].astype(F32)
    back = forward_ref[...].astype(F32) - times(picked.astype(BF16), edge_ref[...])
    back = back.astype(BF16)
    chunks = chunks_of(factor_ref.shape[0])
    for first, rows in chunks:
        total = None
        for lower, size in chunks:
            if lower >= first:
                factor = factor_ref[pl.ds(lower, size), pl.ds(first, rows)]
                part = times(back[:, lower : lower + size], factor)
                total = part if total is None else total + part
        out_ref[0, 0, pl.ds(first, rows), :] = total.T.astype(BF16)


def mid_out_kernel(*refs):
    total = refs[0][...].astype(F32)
    for term in refs[1:-1]:
        total = total + term[...].astype(F32)
    refs[-1][0] = total.T.astype(BF16)


def call(kernel, name, inputs, outs, scratch=(), flops=0, space=pltpu.VMEM):
    vmem = pl.BlockSpec(memory_space=pltpu.VMEM)
    smem = pl.BlockSpec(memory_space=pltpu.SMEM)
    in_specs = [smem if x.dtype == jnp.int32 else vmem for x in inputs]
    out_shape = [jax.ShapeDtypeStruct(shape, dtype) for shape, dtype in outs]
    if space == pltpu.HBM:
        in_specs = [pl.BlockSpec(memory_space=space)] * len(inputs)
        inputs = [pltpu.with_memory_space_constraint(x, space) for x in inputs]
        out_shape = [
            (pltpu.SMEM if dtype == jnp.int32 else pltpu.VMEM)(shape, dtype)
            for shape, dtype in outs
        ]
    moved = sum(x.size * x.dtype.itemsize for x in inputs)
    return pl.pallas_call(
        kernel,
        name=name,
        in_specs=in_specs,
        out_specs=[smem if dtype == jnp.int32 else vmem for _, dtype in outs],
        out_shape=out_shape,
        scratch_shapes=list(scratch),
        compiler_params=pltpu.CompilerParams(vmem_limit_bytes=VMEM_LIMIT),
        cost_estimate=pl.CostEstimate(flops=flops, bytes_accessed=moved, transcendentals=0),
    )(*inputs)


def total_of(first, others):
    total = first.astype(F32)
    for other in others:
        total = total + other.astype(F32)
    return total.astype(BF16)


def chips_of(groups, rows_out):
    chips = groups // 2
    return chips if is_split(chips) and rows_out % (2 * BLOCK) == 0 else 1


def group_sum(mine, other, size, chips):
    if not is_split(chips):
        total = total_of(mine[0], [exchange(other[0], "group", 1, size)])
        total = total_of(total, [exchange(total, "group", k, size) for k in range(2, size, 2)])
        return [total], [exchange(total, "group", 1, size)]
    own_units, other_units = [], []
    for kept, given in zip(mine, other):
        rows = kept.shape[1] // 2
        block = rows // 2
        low, high = split(kept, rows)
        low_core, high_core = split(exchange(given, "group", 1, size), rows)
        pair = exchange(total_of(high, [high_core]), "group", 2, size)
        side = total_of(low, [low_core, pair])
        far, near = split(exchange(side, "group", 4, size), block)
        unit = total_of(side, [jnp.concatenate([near, far], axis=1)])
        rest = exchange(unit, "group", 2, size)
        own_units += [unit, rest]
        other_units += [exchange(unit, "group", 1, size), exchange(rest, "group", 1, size)]
    return own_units, other_units


def member_sum(low, high, size):
    if not is_power_of_two(size):
        return lax.psum(low, "member"), lax.psum(high, "member")
    steps = [1 << i for i in range(size.bit_length() - 1)]
    for first, second in zip(steps, reversed(steps)):
        other_low = exchange(low, "member", first, size)
        other_high = exchange(high, "member", second, size)
        low, high = total_of(low, [other_low]), total_of(high, [other_high])
    return low, high


def split(values, rows):
    return values[:, :rows], values[:, rows:]


def scatter_sum(pieces, size):
    rows = pieces[0][0].shape[1]
    if size != 4:
        arrived = [
            split(exchange(jnp.concatenate(pair, axis=1), "member", k, size), rows)
            for k, pair in enumerate(pieces, start=1)
        ]
        return [low for low, _ in arrived], [high for _, high in arrived]
    (low1, high1), (low2, high2), (low3, high3) = pieces
    relay1 = exchange(low3, "member", 1, size)
    relay2 = exchange(high3, "member", 2, size)
    first1 = exchange(low1, "member", 1, size)
    first2 = exchange(high2, "member", 2, size)
    last2 = exchange(total_of(low2, [relay1]), "member", 2, size)
    last1 = exchange(total_of(high1, [relay2]), "member", 1, size)
    return [first1, last2], [first2, last1]


def gather(low, high, size):
    rows = low.shape[1]
    if size != 4:
        values = jnp.concatenate([low, high], axis=1)
        return [(low, high)] + [
            split(exchange(values, "member", k, size), rows) for k in range(1, size)
        ]
    high1 = exchange(high, "member", 1, size)
    low2 = exchange(low, "member", 2, size)
    low1 = exchange(low, "member", 1, size)
    high2 = exchange(high, "member", 2, size)
    low3 = exchange(low2, "member", 1, size)
    high3 = exchange(high1, "member", 2, size)
    return [(low, high), (low1, high1), (low2, high2), (low3, high3)]


def make_on_device(groups, members):
    steps = range(1, members)

    def on_device(
        rhs,
        leaf_pivot_inverse,
        leaf_border_block,
        leaf_map,
        mid_inverse,
        mid_border,
        root_map,
        root_inverse,
    ):
        columns = rhs.shape[3]
        leaf_pivots = rhs.shape[2]
        leaf_rows = leaf_border_block.shape[2]
        own_pivots, pivots = mid_inverse.shape[1:]
        border_rows = mid_border.shape[1]
        own_border = border_rows // members
        row_count, share_rows = root_inverse.shape
        half = share_rows // 2
        rows_out = share_rows // groups

        def flat(rows, dtype=BF16):
            return ((columns, rows), dtype)

        def spread_over_members(values):
            return [values] + [exchange(values, "member", k, members) for k in steps]

        leaf_forward, leaf_factor, leaf_edge, leaf_map, root_map = call(
            leaf_forward_kernel,
            "leaf_forward",
            [rhs, leaf_pivot_inverse, leaf_border_block, leaf_map, root_map],
            [
                flat(leaf_pivots),
                (leaf_pivot_inverse.shape[2:], BF16),
                (leaf_border_block.shape[2:], BF16),
                (leaf_map.shape, jnp.int32),
                (root_map.shape, jnp.int32),
            ],
            [
                pltpu.VMEM((leaf_pivots, columns), BF16),
                pltpu.SemaphoreType.DMA((4 + len(chunks_of(leaf_pivots)),)),
            ],
            flops=2 * columns * leaf_pivots * leaf_pivots,
            space=pltpu.HBM,
        )
        (leaf_out,) = call(
            leaf_out_kernel,
            "leaf_out",
            [leaf_forward, leaf_edge],
            [flat(leaf_rows)],
            flops=PREFETCH_FLOPS,
        )
        terms = spread_over_members(leaf_out)
        mid_forward = []
        groups_of_terms = [[0], list(steps)]
        if members == 4:
            groups_of_terms = [[0], [3], [2, 1]]
        for i, which in enumerate(groups_of_terms):
            last = which is groups_of_terms[-1]
            mid_forward = call(
                functools.partial(mid_forward_kernel, members, which),
                f"mid_forward_{i}",
                [leaf_map, mid_inverse, *(terms[k] for k in which), *mid_forward],
                [flat(own_pivots, BF16 if last else F32)],
                flops=2 * columns * own_pivots * leaf_rows * len(which),
            )
        (mid_forward,) = mid_forward
        half_border = own_border // 2
        pieces = {
            k: call(
                functools.partial(mid_piece_kernel, members, k),
                f"mid_piece_{k}",
                [mid_border, mid_forward],
                [flat(half_border), flat(half_border)],
                flops=2 * columns * own_pivots * own_border,
            )
            for k in reversed(steps)
        }
        lows, highs = scatter_sum([pieces[k] for k in steps], members)
        (own_update,) = call(
            functools.partial(own_update_kernel, members, pivots // BLOCK),
            "own_update",
            [leaf_map, mid_border, mid_forward, *terms],
            [flat(own_border, F32)],
            flops=2 * columns * own_pivots * own_border,
        )
        chips = chips_of(groups, rows_out)
        whole_share = pltpu.VMEM((columns, share_rows), BF16)
        half_streams = [flat(half // 2)] * 2 if is_split(chips) else [flat(half)]
        count = len(half_streams)
        streams = call(
            functools.partial(root_term_kernel, chips, len(lows)),
            "root_term",
            [root_map, own_update, *lows, *highs],
            half_streams * 2,
            [whole_share],
        )
        units = group_sum(streams[count:], streams[:count], groups, chips)
        if is_split(chips):
            waves = [
                [(1, 0), (1, 2)],
                [(0, 0), (0, 2), (1, 1)],
                [(1, 3), (0, 1)],
                [(0, 3)],
            ]
        else:
            waves = [[(1, 0)], [(0, 0)]]
        root_flops = columns * row_count * share_rows
        half_count = row_count // 2
        before = []
        for i, which in enumerate(waves[:-1]):
            before = call(
                functools.partial(root_early_kernel, chips, which),
                f"root_early_{i}",
                [root_inverse, *(units[1 - own][k] for own, k in which), *before],
                [flat(half_count, F32), flat(half_count, F32)],
                flops=root_flops // 2,
            )
        root_parts = [
            call(
                functools.partial(root_forward_kernel, chips, waves[-1], part),
                f"root_forward_{part}",
                [root_inverse, *(units[1 - own][k] for own, k in waves[-1]), total],
                [flat(half_count)],
                flops=root_flops // 4,
            )[0]
            for part, total in enumerate(before)
        ]
        root_forward = member_sum(*root_parts, members)
        halves = {}
        for own in (False, True):
            before = []
            for part, forward in enumerate(root_forward):
                before = call(
                    functools.partial(root_back_kernel, chips, own, part),
                    f"root_back_{own}_{part}",
                    [root_inverse, forward, *before],
                    [(shape, BF16 if part else F32) for shape, _ in half_streams],
                    flops=root_flops // 2,
                )
            halves[own] = before
        mine, other = group_sum(halves[True], halves[False], groups, chips)
        own_values = call(
            functools.partial(root_pick_kernel, chips),
            "root_pick",
            [root_map, *mine, *other],
            [flat(half_border), flat(half_border)],
            [whole_share],
        )
        shape = [((1, rows_out, columns), BF16)]
        if is_split(chips):
            (root_out,) = call(root_out_kernel, "root_out", [mine[0], mine[2]], shape)
        else:
            turned = pltpu.VMEM((max(rows_out, BLOCK), columns), F32)
            (root_out,) = call(
                root_slice_kernel, "root_slice", [*mine, *other], shape, [whole_share, turned]
            )
        values = gather(*own_values, members)
        if members == 4:
            waves = [[(0, 0), (0, 1), (1, 1), (2, 0)], [(1, 0), (2, 1)], [(3, 0), (3, 1)]]
        else:
            waves = [[(0, 0), (0, 1)], [(k, h) for k in steps for h in range(2)]]
        back = mid_forward
        for i, which in enumerate(waves[:-1]):
            (back,) = call(
                functools.partial(mid_early_kernel, members, which),
                f"mid_early_{i}",
                [mid_border, back] + [values[k][h] for k, h in which],
                [flat(own_pivots, F32)],
                flops=2 * columns * own_pivots * half_border * len(which),
            )
        part, *last_pair = call(
            functools.partial(mid_back_kernel, members, waves[-1]),
            "mid_back",
            [leaf_map, mid_inverse, mid_border, back] + [values[k][h] for k, h in waves[-1]],
            [flat(pivots), flat(leaf_rows), flat(own_pivots)],
            flops=2 * columns * own_pivots * (pivots + half_border * len(waves[-1])),
        )
        pairs = [
            call(
                functools.partial(mid_share_kernel, members, k),
                f"mid_share_{k}",
                [leaf_map, part],
                [flat(leaf_rows), flat(own_pivots)],
                flops=SHARE_FLOPS,
            )
            for k in steps[:-1]
        ]
        picked, pieces = scatter_sum([*pairs, last_pair], members)
        base, own_piece = call(
            functools.partial(pick_kernel, members),
            "pick",
            [leaf_map, part] + [half for pair in values for half in pair],
            [flat(leaf_rows), flat(own_pivots)],
            flops=SHARE_FLOPS,
        )
        (leaf_values,) = call(
            leaf_back_kernel,
            "leaf_back",
            [leaf_factor, leaf_edge, leaf_forward, base, *picked],
            [((1, 1, leaf_pivots, columns), BF16)],
            flops=2 * columns * leaf_pivots * (leaf_pivots + leaf_rows),
        )
        (mid_out,) = call(
            mid_out_kernel, "mid_out", [own_piece, *pieces], [((1, own_pivots, columns), BF16)]
        )
        return leaf_values, mid_out, root_out

    return on_device


def solution(mesh):
    in_specs = (
        P("group", "member", None, None),
        P("group", "member", None, None),
        P("group", "member", None, None),
        P("group", None, None),
        P("group", "member", None),
        P("group", None, "member"),
        P("group", "member", None),
        P("group", "member"),
    )
    out_specs = (
        P("group", "member", None, None),
        P("group", "member", None),
        P("member", "group", None),
    )
    on_device = make_on_device(mesh.shape["group"], mesh.shape["member"])
    return jax.shard_map(
        on_device, mesh=mesh, in_specs=in_specs, out_specs=out_specs, check_vma=False
    )
```

```python
import functools

import jax
import jax.numpy as jnp
from jax import lax
from jax.experimental import pallas as pl
from jax.experimental.pallas import tpu as pltpu
from jax.sharding import PartitionSpec as P


BLOCK = 128
VMEM_LIMIT = 20 * 1024 * 1024
PREFETCH_FLOPS = 2 * 10**10
SHARE_FLOPS = 2 * 10**8
F32 = jnp.float32
BF16 = jnp.bfloat16


def is_power_of_two(size):
    return size & (size - 1) == 0


def partner(index, step, size):
    return index ^ step if is_power_of_two(size) else (index + step) % size


def exchange(values, axis, step, size):
    return lax.ppermute(values, axis, [(i, partner(i, step, size)) for i in range(size)])


def times_transpose(values, matrix):
    return lax.dot_general(values, matrix, (((1,), (1,)), ((), ())), preferred_element_type=F32)


def times(values, matrix):
    return jnp.dot(values, matrix, preferred_element_type=F32)


def traced_source(index, step, size):
    if is_power_of_two(size):
        return lax.bitwise_xor(index, jnp.int32(step))
    return lax.rem(index - step + size, jnp.int32(size))


def traced_partner(index, step, size):
    if is_power_of_two(size):
        return lax.bitwise_xor(index, jnp.int32(step))
    return lax.rem(index + step, jnp.int32(size))


def at_block(index):
    return pl.ds(pl.multiple_of(index * BLOCK, BLOCK), BLOCK)


def at_part(index, size):
    return pl.ds(pl.multiple_of(index * size, BLOCK), size)


def static_block(index):
    return pl.ds(index * BLOCK, BLOCK)


def chunks_of(size):
    rows = 2 * BLOCK if size % (2 * BLOCK) == 0 else size
    return [(first, rows) for first in range(0, size, rows)]


def leaf_forward_kernel(
    rhs_hbm,
    factor_hbm,
    edge_hbm,
    leaf_map_hbm,
    root_map_hbm,
    forward_ref,
    factor_ref,
    edge_ref,
    leaf_map_ref,
    root_map_ref,
    rhs_ref,
    sems,
):
    chunks = chunks_of(factor_ref.shape[0])
    copies = [pltpu.make_async_copy(rhs_hbm.at[0, 0], rhs_ref, sems.at[0])]
    for i, (first, rows) in enumerate(chunks, start=1):
        part = (pl.ds(first, rows), pl.ds(0, first + rows))
        copies.append(
            pltpu.make_async_copy(factor_hbm.at[0, 0, *part], factor_ref.at[*part], sems.at[i])
        )
    later = [
        pltpu.make_async_copy(source_ref, target_ref, sems.at[1 + len(chunks) + i])
        for i, (source_ref, target_ref) in enumerate(
            (
                (edge_hbm.at[0, 0], edge_ref),
                (leaf_map_hbm, leaf_map_ref),
                (root_map_hbm, root_map_ref),
            )
        )
    ]
    for copy in copies + later:
        copy.start()
    copies[0].wait()
    source_rows = rhs_ref[...].T
    for copy, (first, rows) in zip(copies[1:], chunks):
        copy.wait()
        factor = factor_ref[pl.ds(first, rows), pl.ds(0, first + rows)]
        forward = times_transpose(source_rows[:, : first + rows], factor)
        forward_ref[:, pl.ds(first, rows)] = forward.astype(BF16)
    for copy in later:
        copy.wait()


def leaf_out_kernel(forward_ref, edge_ref, out_ref):
    out_ref[...] = (-times_transpose(forward_ref[...], edge_ref[...])).astype(BF16)


def border_piece(border_ref, owner, rows):
    return border_ref[0, pl.ds(pl.multiple_of(owner * rows, BLOCK), rows), :]


def mid_forward_kernel(members, which, map_ref, inverse_ref, *refs):
    forward_ref = refs[-1]
    terms = refs[: len(which)]
    before = refs[len(which) : -1]
    pivot_blocks = inverse_ref.shape[2] // BLOCK
    member = lax.axis_index("member")
    total = before[0][...] if before else None
    for k, term in zip(which, terms):
        owner = traced_source(member, k, members)
        blocks = range(term.shape[1] // BLOCK)
        for first in blocks[::2]:
            values, columns = [], []
            for j in blocks[first : first + 2]:
                target = map_ref[0, owner, j]
                block = term[:, static_block(j)]
                values.append(jnp.where(target < pivot_blocks, block, jnp.zeros_like(block)))
                columns.append(inverse_ref[0, :, at_block(lax.min(target, pivot_blocks - 1))])
            part = times_transpose(
                jnp.concatenate(values, axis=1), jnp.concatenate(columns, axis=1)
            )
            total = part if total is None else total + part
    forward_ref[...] = total.astype(forward_ref.dtype)


def mid_piece_kernel(members, step, border_ref, forward_ref, low_ref, high_ref):
    owner = traced_partner(lax.axis_index("member"), step, members)
    rows = low_ref.shape[1]
    for half, ref in enumerate((low_ref, high_ref)):
        piece = border_piece(border_ref, 2 * owner + half, rows)
        ref[...] = (-times_transpose(forward_ref[...], piece)).astype(BF16)


def own_update_kernel(members, pivot_blocks, *refs):
    map_ref, border_ref, forward_ref = refs[:3]
    terms = refs[3 : 3 + members]
    update_ref = refs[-1]
    member = lax.axis_index("member")
    rows = update_ref.shape[1]
    piece = border_ref[0, pl.ds(pl.multiple_of(member * rows, BLOCK), rows), :]
    update_ref[...] = -times_transpose(forward_ref[...], piece)
    first = pivot_blocks + member * (rows // BLOCK)
    for k, term in enumerate(terms):
        owner = traced_source(member, k, members)
        for j in range(term.shape[1] // BLOCK):
            target = map_ref[0, owner, j] - first

            @pl.when((target >= 0) & (target < rows // BLOCK))
            def _():
                update_ref[:, at_block(target)] += term[:, static_block(j)].astype(F32)


DISTANCES = (0, 2, 1, 3)


def is_split(chips):
    return chips == len(DISTANCES)


def stream_places(core, chips, share):
    if not is_split(chips):
        return [[core * (share // 2)]], share // 2
    chip = lax.axis_index("group") // 2
    size = share // (4 * chips)
    owners = [2 * lax.bitwise_xor(chip, jnp.int32(k)) + core for k in DISTANCES]
    return [[(2 * owner + stream) * size for owner in owners] for stream in range(2)], size


def unit_places(core, chips, share):
    streams, size = stream_places(core, chips, share)
    if not is_split(chips):
        return streams, size
    return [places[i : i + 2] for places in streams for i in (0, 2)], size


def at_places(ref, lines, places, size):
    parts = [ref[lines, pl.ds(pl.multiple_of(place, BLOCK), size)] for place in places]
    return parts[0] if len(parts) == 1 else jnp.concatenate(parts, axis=1)


def take_streams(refs, spread, core, chips):
    streams, size = stream_places(core, chips, spread.shape[1])
    for ref, places in zip(refs, streams):
        for i, place in enumerate(places):
            ref[:, pl.ds(i * size, size)] = spread[:, pl.ds(pl.multiple_of(place, BLOCK), size)]


def root_term_kernel(chips, lows, *refs):
    count = 2 if is_split(chips) else 1
    inputs, outs, spread = refs[: -1 - 2 * count], refs[-1 - 2 * count : -1], refs[-1]
    map_ref, own_ref = inputs[:2]
    arrived = (inputs[2 : 2 + lows], inputs[2 + lows :])
    core = lax.axis_index("group") & 1
    spread[...] = jnp.zeros_like(spread)
    half_blocks = own_ref.shape[1] // (2 * BLOCK)
    for i in range(2 * half_blocks):
        total = own_ref[:, static_block(i)]
        for term in arrived[i // half_blocks]:
            total = total + term[:, static_block(i % half_blocks)].astype(F32)
        spread[:, at_block(map_ref[0, 0, i])] = total.astype(BF16)
    take_streams(outs[:count], spread, 1 - core, chips)
    take_streams(outs[count:], spread, core, chips)


def join(joined, units, chips):
    core = lax.axis_index("group") & 1
    count = len(units) // 2
    for owner, refs in ((core, units[:count]), (1 - core, units[count:])):
        places_of, size = unit_places(owner, chips, joined.shape[1])
        for ref, places in zip(refs, places_of):
            for i, place in enumerate(places):
                target = pl.ds(pl.multiple_of(place, BLOCK), size)
                joined[:, target] = ref[:, pl.ds(i * size, size)]


def root_product(chips, which, units, inverse_ref, lines):
    core = lax.axis_index("group") & 1
    total = None
    for (own, number), ref in zip(which, units):
        places_of, size = unit_places(core if own else 1 - core, chips, inverse_ref.shape[1])
        columns = at_places(inverse_ref, lines, places_of[number], size)
        part = times_transpose(ref[...], columns)
        total = part if total is None else total + part
    return total


def root_early_kernel(chips, which, inverse_ref, *refs):
    units, before, outs = refs[: len(which)], refs[len(which) : -2], refs[-2:]
    rows = outs[0].shape[1]
    for part, out_ref in enumerate(outs):
        total = root_product(chips, which, units, inverse_ref, pl.ds(part * rows, rows))
        out_ref[...] = total + before[part][...] if before else total


def root_forward_kernel(chips, which, part, inverse_ref, *refs):
    units, before_ref, out_ref = refs[:-2], refs[-2], refs[-1]
    rows = out_ref.shape[1]
    total = root_product(chips, which, units, inverse_ref, pl.ds(part * rows, rows))
    out_ref[...] = (total + before_ref[...]).astype(BF16)


def root_back_kernel(chips, owners, part, inverse_ref, forward_ref, *refs):
    count = len(owners) * (2 if is_split(chips) else 1)
    before, outs = refs[:-count], refs[-count:]
    core = lax.axis_index("group") & 1
    places_of = []
    for own in owners:
        streams, size = stream_places(core if own else 1 - core, chips, inverse_ref.shape[1])
        places_of += streams
    forward = forward_ref[...]
    lines = pl.ds(part * forward.shape[1], forward.shape[1])
    for i, (places, out_ref) in enumerate(zip(places_of, outs)):
        total = times(forward, at_places(inverse_ref, lines, places, size))
        if before:
            total = total + before[i][...]
        out_ref[...] = total.astype(out_ref.dtype)


def root_pick_kernel(chips, map_ref, *refs):
    units, (low_ref, high_ref, joined) = refs[:-3], refs[-3:]
    join(joined, units, chips)
    blocks = low_ref.shape[1] // BLOCK
    for i in range(2 * blocks):
        ref = (low_ref, high_ref)[i // blocks]
        ref[:, static_block(i % blocks)] = joined[:, at_block(map_ref[0, 0, i])]


def root_out_kernel(low_ref, high_ref, out_ref):
    rows = out_ref.shape[1] // 2
    for i, ref in enumerate((low_ref, high_ref)):
        out_ref[0, pl.ds(i * rows, rows), :] = ref[:, pl.ds(0, rows)].T


def root_slice_kernel(mine_ref, other_ref, out_ref, joined, turned):
    join(joined, (mine_ref, other_ref), 1)
    rows_out = out_ref.shape[1]
    first = lax.axis_index("group") * rows_out
    rows = turned.shape[0]
    turned[...] = joined[:, at_part(first // rows, rows)].astype(F32).T
    begin = pl.multiple_of(lax.rem(first, jnp.int32(rows)), min(rows_out, rows))
    out_ref[0] = turned[pl.ds(begin, rows_out), :].astype(BF16)


def border_product(members, values, which, border_ref):
    member = lax.axis_index("member")
    total = None
    for (step, half), ref in zip(which, values):
        owner = traced_source(member, step, members)
        piece = border_piece(border_ref, 2 * owner + half, ref.shape[1])
        part = times(ref[...], piece)
        total = part if total is None else total + part
    return total


def mid_early_kernel(members, which, border_ref, back_ref, *refs):
    product = border_product(members, refs[:-1], which, border_ref)
    refs[-1][...] = back_ref[...].astype(F32) - product


def ask(map_ref, owner, part_ref, out_ref):
    pivot_blocks = part_ref.shape[1] // BLOCK
    for j in range(out_ref.shape[1] // BLOCK):
        target = map_ref[0, owner, j]
        block = part_ref[:, at_block(lax.min(target, pivot_blocks - 1))]
        out_ref[:, static_block(j)] = jnp.where(
            target < pivot_blocks, block, jnp.zeros_like(block)
        )


def mid_back_kernel(members, late, map_ref, inverse_ref, border_ref, back_ref, *refs):
    values = refs[:-3]
    part_ref, asked_ref, piece_ref = refs[-3:]
    back = back_ref[...] - border_product(members, values, late, border_ref)
    part_ref[...] = times(back.astype(BF16), inverse_ref[0]).astype(BF16)
    owner = traced_partner(lax.axis_index("member"), members - 1, members)
    ask(map_ref, owner, part_ref, asked_ref)
    piece_ref[...] = part_ref[:, at_part(owner, piece_ref.shape[1])]


def mid_share_kernel(members, step, map_ref, part_ref, asked_ref, piece_ref):
    owner = traced_partner(lax.axis_index("member"), step, members)
    ask(map_ref, owner, part_ref, asked_ref)
    piece_ref[...] = part_ref[:, at_part(owner, piece_ref.shape[1])]


def pick_kernel(members, map_ref, part_ref, *refs):
    values = refs[:-2]
    base_ref, own_ref = refs[-2:]
    member = lax.axis_index("member")
    pivot_blocks = part_ref.shape[1] // BLOCK
    rows = values[0].shape[1]
    for j in range(base_ref.shape[1] // BLOCK):
        target = map_ref[0, member, j]

        @pl.when(target < pivot_blocks)
        def _():
            base_ref[:, static_block(j)] = part_ref[:, at_block(target)]

        border = target - pivot_blocks
        for k, values_ref in enumerate(values):
            owner = traced_source(member, k // 2, members)
            inner = border - (2 * owner + k % 2) * (rows // BLOCK)

            @pl.when((border >= 0) & (inner >= 0) & (inner < rows // BLOCK))
            def _():
                base_ref[:, static_block(j)] = values_ref[:, at_block(inner)]

    own_ref[...] = part_ref[:, at_part(member, own_ref.shape[1])]


def leaf_back_kernel(*refs):
    factor_ref, edge_ref, forward_ref = refs[:3]
    terms = refs[3:-1]
    out_ref = refs[-1]
    picked = terms[0][...].astype(F32)
    for term in terms[1:]:
        picked = picked + term[...].astype(F32)
    back = forward_ref[...].astype(F32) - times(picked.astype(BF16), edge_ref[...])
    back = back.astype(BF16)
    chunks = chunks_of(factor_ref.shape[0])
    for first, rows in chunks:
        total = None
        for lower, size in chunks:
            if lower >= first:
                factor = factor_ref[pl.ds(lower, size), pl.ds(first, rows)]
                part = times(back[:, lower : lower + size], factor)
                total = part if total is None else total + part
        out_ref[0, 0, pl.ds(first, rows), :] = total.astype(BF16).T


def mid_out_kernel(*refs):
    total = refs[0][...].astype(F32)
    for term in refs[1:-1]:
        total = total + term[...].astype(F32)
    refs[-1][0] = total.astype(BF16).T


def call(kernel, inputs, outs, scratch=(), flops=0, space=pltpu.VMEM):
    vmem = pl.BlockSpec(memory_space=pltpu.VMEM)
    smem = pl.BlockSpec(memory_space=pltpu.SMEM)
    in_specs = [smem if x.dtype == jnp.int32 else vmem for x in inputs]
    out_shape = [jax.ShapeDtypeStruct(shape, dtype) for shape, dtype in outs]
    if space == pltpu.HBM:
        in_specs = [pl.BlockSpec(memory_space=space)] * len(inputs)
        inputs = [pltpu.with_memory_space_constraint(x, space) for x in inputs]
        out_shape = [
            (pltpu.SMEM if dtype == jnp.int32 else pltpu.VMEM)(shape, dtype)
            for shape, dtype in outs
        ]
    moved = sum(x.size * x.dtype.itemsize for x in inputs)
    return pl.pallas_call(
        kernel,
        in_specs=in_specs,
        out_specs=[smem if dtype == jnp.int32 else vmem for _, dtype in outs],
        out_shape=out_shape,
        scratch_shapes=list(scratch),
        compiler_params=pltpu.CompilerParams(vmem_limit_bytes=VMEM_LIMIT),
        cost_estimate=pl.CostEstimate(flops=flops, bytes_accessed=moved, transcendentals=0),
    )(*inputs)


def total_of(first, others):
    total = first.astype(F32)
    for other in others:
        total = total + other.astype(F32)
    return total.astype(BF16)


def chips_of(groups, rows_out):
    chips = groups // 2
    return chips if is_split(chips) and rows_out % (2 * BLOCK) == 0 else 1


def group_sum(mine, other, size, chips):
    if not is_split(chips):
        total = total_of(mine[0], [exchange(other[0], "group", 1, size)])
        total = total_of(total, [exchange(total, "group", k, size) for k in range(2, size, 2)])
        return [total], [exchange(total, "group", 1, size)]
    own_units, other_units = [], []
    for kept, given in zip(mine, other):
        rows = kept.shape[1] // 2
        block = rows // 2
        low, high = split(kept, rows)
        low_core, high_core = split(exchange(given, "group", 1, size), rows)
        pair = exchange(total_of(high, [high_core]), "group", 2, size)
        side = total_of(low, [low_core, pair])
        far, near = split(exchange(side, "group", 4, size), block)
        unit = total_of(side, [jnp.concatenate([near, far], axis=1)])
        rest = exchange(unit, "group", 2, size)
        own_units += [unit, rest]
        other_units += [exchange(unit, "group", 1, size), exchange(rest, "group", 1, size)]
    return own_units, other_units


def member_sum(low, high, size):
    if not is_power_of_two(size):
        return lax.psum(low, "member"), lax.psum(high, "member")
    steps = [1 << i for i in range(size.bit_length() - 1)]
    for first, second in zip(steps, reversed(steps)):
        other_low = exchange(low, "member", first, size)
        other_high = exchange(high, "member", second, size)
        low, high = total_of(low, [other_low]), total_of(high, [other_high])
    return low, high


def split(values, rows):
    return values[:, :rows], values[:, rows:]


def scatter_sum(pieces, size):
    rows = pieces[0][0].shape[1]
    if size != 4:
        arrived = [
            split(exchange(jnp.concatenate(pair, axis=1), "member", k, size), rows)
            for k, pair in enumerate(pieces, start=1)
        ]
        return [low for low, _ in arrived], [high for _, high in arrived]
    (low1, high1), (low2, high2), (low3, high3) = pieces
    relay1 = exchange(low3, "member", 1, size)
    relay2 = exchange(high3, "member", 2, size)
    first1 = exchange(low1, "member", 1, size)
    first2 = exchange(high2, "member", 2, size)
    last2 = exchange(total_of(low2, [relay1]), "member", 2, size)
    last1 = exchange(total_of(high1, [relay2]), "member", 1, size)
    return [first1, last2], [first2, last1]


def gather(low, high, size):
    rows = low.shape[1]
    if size != 4:
        values = jnp.concatenate([low, high], axis=1)
        return [(low, high)] + [
            split(exchange(values, "member", k, size), rows) for k in range(1, size)
        ]
    high1 = exchange(high, "member", 1, size)
    low2 = exchange(low, "member", 2, size)
    low1 = exchange(low, "member", 1, size)
    high2 = exchange(high, "member", 2, size)
    low3 = exchange(low2, "member", 1, size)
    high3 = exchange(high1, "member", 2, size)
    return [(low, high), (low1, high1), (low2, high2), (low3, high3)]


def make_on_device(groups, members):
    steps = range(1, members)

    def on_device(
        rhs,
        leaf_pivot_inverse,
        leaf_border_block,
        leaf_map,
        mid_inverse,
        mid_border,
        root_map,
        root_inverse,
    ):
        columns = rhs.shape[3]
        leaf_pivots = rhs.shape[2]
        leaf_rows = leaf_border_block.shape[2]
        own_pivots, pivots = mid_inverse.shape[1:]
        border_rows = mid_border.shape[1]
        own_border = border_rows // members
        row_count, share_rows = root_inverse.shape
        half = share_rows // 2
        rows_out = share_rows // groups

        def flat(rows, dtype=BF16):
            return ((columns, rows), dtype)

        def spread_over_members(values):
            return [values] + [exchange(values, "member", k, members) for k in steps]

        leaf_forward, leaf_factor, leaf_edge, leaf_map, root_map = call(
            leaf_forward_kernel,
            [rhs, leaf_pivot_inverse, leaf_border_block, leaf_map, root_map],
            [
                flat(leaf_pivots),
                (leaf_pivot_inverse.shape[2:], BF16),
                (leaf_border_block.shape[2:], BF16),
                (leaf_map.shape, jnp.int32),
                (root_map.shape, jnp.int32),
            ],
            [
                pltpu.VMEM((leaf_pivots, columns), BF16),
                pltpu.SemaphoreType.DMA((4 + len(chunks_of(leaf_pivots)),)),
            ],
            flops=2 * columns * leaf_pivots * leaf_pivots,
            space=pltpu.HBM,
        )
        (leaf_out,) = call(
            leaf_out_kernel, [leaf_forward, leaf_edge], [flat(leaf_rows)], flops=PREFETCH_FLOPS
        )
        terms = spread_over_members(leaf_out)
        mid_forward = []
        groups_of_terms = [[0], list(steps)]
        if members == 4:
            groups_of_terms = [[0], [3], [2, 1]]
        for which in groups_of_terms:
            last = which is groups_of_terms[-1]
            mid_forward = call(
                functools.partial(mid_forward_kernel, members, which),
                [leaf_map, mid_inverse, *(terms[k] for k in which), *mid_forward],
                [flat(own_pivots, BF16 if last else F32)],
                flops=2 * columns * own_pivots * leaf_rows * len(which),
            )
        (mid_forward,) = mid_forward
        half_border = own_border // 2
        pieces = {
            k: call(
                functools.partial(mid_piece_kernel, members, k),
                [mid_border, mid_forward],
                [flat(half_border), flat(half_border)],
                flops=2 * columns * own_pivots * own_border,
            )
            for k in reversed(steps)
        }
        lows, highs = scatter_sum([pieces[k] for k in steps], members)
        (own_update,) = call(
            functools.partial(own_update_kernel, members, pivots // BLOCK),
            [leaf_map, mid_border, mid_forward, *terms],
            [flat(own_border, F32)],
            flops=2 * columns * own_pivots * own_border,
        )
        chips = chips_of(groups, rows_out)
        whole_share = pltpu.VMEM((columns, share_rows), BF16)
        half_streams = [flat(half // 2)] * 2 if is_split(chips) else [flat(half)]
        count = len(half_streams)
        streams = call(
            functools.partial(root_term_kernel, chips, len(lows)),
            [root_map, own_update, *lows, *highs],
            half_streams * 2,
            [whole_share],
        )
        units = group_sum(streams[count:], streams[:count], groups, chips)
        if is_split(chips):
            waves = [
                [(1, 0), (1, 2)],
                [(0, 0), (0, 2), (1, 1)],
                [(1, 3), (0, 1)],
                [(0, 3)],
            ]
        else:
            waves = [[(1, 0)], [(0, 0)]]
        root_flops = columns * row_count * share_rows
        half_count = row_count // 2
        before = []
        for which in waves[:-1]:
            before = call(
                functools.partial(root_early_kernel, chips, which),
                [root_inverse, *(units[1 - own][k] for own, k in which), *before],
                [flat(half_count, F32), flat(half_count, F32)],
                flops=root_flops // 2,
            )
        root_parts = [
            call(
                functools.partial(root_forward_kernel, chips, waves[-1], part),
                [root_inverse, *(units[1 - own][k] for own, k in waves[-1]), total],
                [flat(half_count)],
                flops=root_flops // 4,
            )[0]
            for part, total in enumerate(before)
        ]
        root_forward = member_sum(*root_parts, members)
        first = call(
            functools.partial(root_back_kernel, chips, (0, 1), 0),
            [root_inverse, root_forward[0]],
            [(shape, F32) for shape, _ in half_streams * 2],
            flops=root_flops,
        )
        other, mine = (
            call(
                functools.partial(root_back_kernel, chips, (own,), 1),
                [root_inverse, root_forward[1], *first[own * count : (own + 1) * count]],
                half_streams,
                flops=root_flops // 2,
            )
            for own in (0, 1)
        )
        mine, other = group_sum(mine, other, groups, chips)
        own_values = call(
            functools.partial(root_pick_kernel, chips),
            [root_map, *mine, *other],
            [flat(half_border), flat(half_border)],
            [whole_share],
        )
        shape = [((1, rows_out, columns), BF16)]
        if is_split(chips):
            (root_out,) = call(root_out_kernel, [mine[0], mine[2]], shape)
        else:
            turned = pltpu.VMEM((max(rows_out, BLOCK), columns), F32)
            (root_out,) = call(root_slice_kernel, [*mine, *other], shape, [whole_share, turned])
        values = gather(*own_values, members)
        if members == 4:
            waves = [[(0, 0), (0, 1), (1, 1), (2, 0)], [(1, 0), (2, 1)], [(3, 0), (3, 1)]]
        else:
            waves = [[(0, 0), (0, 1)], [(k, h) for k in steps for h in range(2)]]
        back = mid_forward
        for which in waves[:-1]:
            (back,) = call(
                functools.partial(mid_early_kernel, members, which),
                [mid_border, back] + [values[k][h] for k, h in which],
                [flat(own_pivots, F32)],
                flops=2 * columns * own_pivots * half_border * len(which),
            )
        part, *last_pair = call(
            functools.partial(mid_back_kernel, members, waves[-1]),
            [leaf_map, mid_inverse, mid_border, back] + [values[k][h] for k, h in waves[-1]],
            [flat(pivots), flat(leaf_rows), flat(own_pivots)],
            flops=2 * columns * own_pivots * (pivots + half_border * len(waves[-1])),
        )
        pairs = [
            call(
                functools.partial(mid_share_kernel, members, k),
                [leaf_map, part],
                [flat(leaf_rows), flat(own_pivots)],
                flops=SHARE_FLOPS,
            )
            for k in steps[:-1]
        ]
        picked, pieces = scatter_sum([*pairs, last_pair], members)
        base, own_piece = call(
            functools.partial(pick_kernel, members),
            [leaf_map, part] + [half for pair in values for half in pair],
            [flat(leaf_rows), flat(own_pivots)],
            flops=SHARE_FLOPS,
        )
        (leaf_values,) = call(
            leaf_back_kernel,
            [leaf_factor, leaf_edge, leaf_forward, base, *picked],
            [((1, 1, leaf_pivots, columns), BF16)],
            flops=2 * columns * leaf_pivots * (leaf_pivots + leaf_rows),
        )
        (mid_out,) = call(mid_out_kernel, [own_piece, *pieces], [((1, own_pivots, columns), BF16)])
        return leaf_values, mid_out, root_out

    return on_device


def solution(mesh):
    in_specs = (
        P("group", "member", None, None),
        P("group", "member", None, None),
        P("group", "member", None, None),
        P("group", None, None),
        P("group", "member", None),
        P("group", None, "member"),
        P("group", "member", None),
        P("group", "member"),
    )
    out_specs = (
        P("group", "member", None, None),
        P("group", "member", None),
        P("member", "group", None),
    )
    on_device = make_on_device(mesh.shape["group"], mesh.shape["member"])

    return jax.shard_map(
        on_device, mesh=mesh, in_specs=in_specs, out_specs=out_specs, check_vma=False
    )
```

```python
import functools

import jax
import jax.numpy as jnp
from jax import lax
from jax.experimental import pallas as pl
from jax.experimental.pallas import tpu as pltpu
from jax.sharding import PartitionSpec as P


BLOCK = 128
VMEM_LIMIT = 20 * 1024 * 1024
PREFETCH_FLOPS = 2 * 10**10
SHARE_FLOPS = 2 * 10**8
F32 = jnp.float32
BF16 = jnp.bfloat16
GROUP, MEMBER = "group", "member"


def is_power_of_two(size):
    return size & (size - 1) == 0


def partner(index, step, size):
    return index ^ step if is_power_of_two(size) else (index + step) % size


def exchange(values, axis, step, size):
    return lax.ppermute(values, axis, [(i, partner(i, step, size)) for i in range(size)])


def times_transpose(values, matrix):
    return lax.dot_general(values, matrix, (((1,), (1,)), ((), ())), preferred_element_type=F32)


def times(values, matrix):
    return jnp.dot(values, matrix, preferred_element_type=F32)


def traced_source(index, step, size):
    if is_power_of_two(size):
        return lax.bitwise_xor(index, jnp.int32(step))
    return lax.rem(index - step + size, jnp.int32(size))


def traced_partner(index, step, size):
    if is_power_of_two(size):
        return lax.bitwise_xor(index, jnp.int32(step))
    return lax.rem(index + step, jnp.int32(size))


def at_block(index):
    return pl.ds(pl.multiple_of(index * BLOCK, BLOCK), BLOCK)


def at_part(index, size):
    return pl.ds(pl.multiple_of(index * size, BLOCK), size)


def static_block(index):
    return pl.ds(index * BLOCK, BLOCK)


def chunks_of(size):
    rows = 2 * BLOCK if size % (2 * BLOCK) == 0 else size
    return [(first, rows) for first in range(0, size, rows)]


def leaf_forward_kernel(
    rhs_hbm,
    factor_hbm,
    edge_hbm,
    leaf_map_hbm,
    root_map_hbm,
    forward_ref,
    factor_ref,
    edge_ref,
    leaf_map_ref,
    root_map_ref,
    rhs_ref,
    sems,
):
    chunks = chunks_of(factor_ref.shape[0])
    copies = [pltpu.make_async_copy(rhs_hbm.at[0, 0], rhs_ref, sems.at[0])]
    for i, (first, rows) in enumerate(chunks, start=1):
        part = (pl.ds(first, rows), pl.ds(0, first + rows))
        copies.append(
            pltpu.make_async_copy(factor_hbm.at[0, 0, *part], factor_ref.at[*part], sems.at[i])
        )
    later = [
        pltpu.make_async_copy(source_ref, target_ref, sems.at[1 + len(chunks) + i])
        for i, (source_ref, target_ref) in enumerate(
            (
                (edge_hbm.at[0, 0], edge_ref),
                (leaf_map_hbm, leaf_map_ref),
                (root_map_hbm, root_map_ref),
            )
        )
    ]
    for copy in copies + later:
        copy.start()
    copies[0].wait()
    source_rows = rhs_ref[...].T
    for copy, (first, rows) in zip(copies[1:], chunks):
        copy.wait()
        factor = factor_ref[pl.ds(first, rows), pl.ds(0, first + rows)]
        forward = times_transpose(source_rows[:, : first + rows], factor)
        forward_ref[:, pl.ds(first, rows)] = forward.astype(BF16)
    for copy in later:
        copy.wait()


def leaf_out_kernel(forward_ref, edge_ref, out_ref):
    out_ref[...] = (-times_transpose(forward_ref[...], edge_ref[...])).astype(BF16)


def border_piece(border_ref, owner, rows):
    return border_ref[0, pl.ds(pl.multiple_of(owner * rows, BLOCK), rows), :]


def mid_forward_kernel(members, which, map_ref, inverse_ref, *refs):
    forward_ref = refs[-1]
    terms = refs[: len(which)]
    before = refs[len(which) : -1]
    pivot_blocks = inverse_ref.shape[2] // BLOCK
    member = lax.axis_index(MEMBER)
    total = before[0][...] if before else None
    for k, term in zip(which, terms):
        owner = traced_source(member, k, members)
        blocks = range(term.shape[1] // BLOCK)
        for first in blocks[::2]:
            values, columns = [], []
            for j in blocks[first : first + 2]:
                target = map_ref[0, owner, j]
                block = term[:, static_block(j)]
                values.append(jnp.where(target < pivot_blocks, block, jnp.zeros_like(block)))
                columns.append(inverse_ref[0, :, at_block(lax.min(target, pivot_blocks - 1))])
            part = times_transpose(
                jnp.concatenate(values, axis=1), jnp.concatenate(columns, axis=1)
            )
            total = part if total is None else total + part
    forward_ref[...] = total.astype(forward_ref.dtype)


def mid_piece_kernel(members, step, halves, border_ref, forward_ref, *outs):
    owner = traced_partner(lax.axis_index(MEMBER), step, members)
    for half, ref in zip(halves, outs):
        piece = border_piece(border_ref, 2 * owner + half, ref.shape[1])
        ref[...] = (-times_transpose(forward_ref[...], piece)).astype(BF16)


def own_update_kernel(members, pivot_blocks, *refs):
    map_ref, border_ref, forward_ref = refs[:3]
    terms = refs[3 : 3 + members]
    update_ref = refs[-1]
    member = lax.axis_index(MEMBER)
    rows = update_ref.shape[1]
    piece = border_ref[0, pl.ds(pl.multiple_of(member * rows, BLOCK), rows), :]
    update_ref[...] = -times_transpose(forward_ref[...], piece)
    first = pivot_blocks + member * (rows // BLOCK)
    for k, term in enumerate(terms):
        owner = traced_source(member, k, members)
        for j in range(term.shape[1] // BLOCK):
            target = map_ref[0, owner, j] - first

            @pl.when((target >= 0) & (target < rows // BLOCK))
            def _():
                update_ref[:, at_block(target)] += term[:, static_block(j)].astype(F32)


DISTANCES = (0, 2, 1, 3)


def is_split(chips):
    return chips == len(DISTANCES)


def stream_places(core, chips, share):
    if not is_split(chips):
        return [[core * (share // 2)]], share // 2
    chip = lax.axis_index(GROUP) // 2
    size = share // (4 * chips)
    owners = [2 * lax.bitwise_xor(chip, jnp.int32(k)) + core for k in DISTANCES]
    return [[(2 * owner + stream) * size for owner in owners] for stream in range(2)], size


def unit_places(core, chips, share):
    streams, size = stream_places(core, chips, share)
    if not is_split(chips):
        return streams, size
    return [places[i : i + 2] for places in streams for i in (0, 2)], size


def at_places(ref, lines, places, size):
    parts = [ref[lines, pl.ds(pl.multiple_of(place, BLOCK), size)] for place in places]
    return parts[0] if len(parts) == 1 else jnp.concatenate(parts, axis=1)


def take_streams(refs, spread, core, chips):
    streams, size = stream_places(core, chips, spread.shape[1])
    for ref, places in zip(refs, streams):
        for i, place in enumerate(places):
            ref[:, pl.ds(i * size, size)] = spread[:, pl.ds(pl.multiple_of(place, BLOCK), size)]


def root_term_kernel(chips, lows, *refs):
    count = 2 if is_split(chips) else 1
    inputs, outs, spread = refs[: -1 - 2 * count], refs[-1 - 2 * count : -1], refs[-1]
    map_ref, own_ref = inputs[:2]
    arrived = (inputs[2 : 2 + lows], inputs[2 + lows :])
    core = lax.axis_index(GROUP) & 1
    spread[...] = jnp.zeros_like(spread)
    half_blocks = own_ref.shape[1] // (2 * BLOCK)
    for i in range(2 * half_blocks):
        total = own_ref[:, static_block(i)]
        for term in arrived[i // half_blocks]:
            total = total + term[:, static_block(i % half_blocks)].astype(F32)
        spread[:, at_block(map_ref[0, 0, i])] = total.astype(BF16)
    take_streams(outs[:count], spread, 1 - core, chips)
    take_streams(outs[count:], spread, core, chips)


def join(joined, units, chips):
    core = lax.axis_index(GROUP) & 1
    count = len(units) // 2
    for owner, refs in ((core, units[:count]), (1 - core, units[count:])):
        places_of, size = unit_places(owner, chips, joined.shape[1])
        for ref, places in zip(refs, places_of):
            for i, place in enumerate(places):
                target = pl.ds(pl.multiple_of(place, BLOCK), size)
                joined[:, target] = ref[:, pl.ds(i * size, size)]


def root_product(chips, which, units, inverse_ref, lines):
    core = lax.axis_index(GROUP) & 1
    total = None
    for (own, number), ref in zip(which, units):
        places_of, size = unit_places(core if own else 1 - core, chips, inverse_ref.shape[1])
        columns = at_places(inverse_ref, lines, places_of[number], size)
        part = times_transpose(ref[...], columns)
        total = part if total is None else total + part
    return total


def root_early_kernel(chips, which, inverse_ref, *refs):
    units, before, outs = refs[: len(which)], refs[len(which) : -2], refs[-2:]
    rows = outs[0].shape[1]
    for part, out_ref in enumerate(outs):
        total = root_product(chips, which, units, inverse_ref, pl.ds(part * rows, rows))
        out_ref[...] = total + before[part][...] if before else total


def root_forward_kernel(chips, which, part, inverse_ref, *refs):
    units, before_ref, out_ref = refs[:-2], refs[-2], refs[-1]
    rows = out_ref.shape[1]
    total = root_product(chips, which, units, inverse_ref, pl.ds(part * rows, rows))
    out_ref[...] = (total + before_ref[...]).astype(BF16)


def root_back_kernel(chips, which, part, inverse_ref, forward_ref, *refs):
    before, outs = refs[: -len(which)], refs[-len(which) :]
    core = lax.axis_index(GROUP) & 1
    forward = forward_ref[...]
    lines = pl.ds(part * forward.shape[1], forward.shape[1])
    for i, ((own, number), out_ref) in enumerate(zip(which, outs)):
        streams, size = stream_places(core if own else 1 - core, chips, inverse_ref.shape[1])
        total = times(forward, at_places(inverse_ref, lines, streams[number], size))
        if before:
            total = total + before[i][...]
        out_ref[...] = total.astype(out_ref.dtype)


def root_pick_kernel(chips, map_ref, *refs):
    units, (low_ref, high_ref, joined) = refs[:-3], refs[-3:]
    join(joined, units, chips)
    blocks = low_ref.shape[1] // BLOCK
    for i in range(2 * blocks):
        ref = (low_ref, high_ref)[i // blocks]
        ref[:, static_block(i % blocks)] = joined[:, at_block(map_ref[0, 0, i])]


def root_out_kernel(low_ref, high_ref, out_ref):
    rows = out_ref.shape[1] // 2
    for i, ref in enumerate((low_ref, high_ref)):
        out_ref[0, pl.ds(i * rows, rows), :] = ref[:, pl.ds(0, rows)].T


def root_slice_kernel(mine_ref, other_ref, out_ref, joined, turned):
    join(joined, (mine_ref, other_ref), 1)
    rows_out = out_ref.shape[1]
    first = lax.axis_index(GROUP) * rows_out
    rows = turned.shape[0]
    turned[...] = joined[:, at_part(first // rows, rows)].astype(F32).T
    begin = pl.multiple_of(lax.rem(first, jnp.int32(rows)), min(rows_out, rows))
    out_ref[0] = turned[pl.ds(begin, rows_out), :].astype(BF16)


def border_product(members, values, which, border_ref):
    member = lax.axis_index(MEMBER)
    total = None
    for (step, half), ref in zip(which, values):
        owner = traced_source(member, step, members)
        piece = border_piece(border_ref, 2 * owner + half, ref.shape[1])
        part = times(ref[...], piece)
        total = part if total is None else total + part
    return total


def mid_early_kernel(members, which, border_ref, back_ref, *refs):
    product = border_product(members, refs[:-1], which, border_ref)
    refs[-1][...] = back_ref[...].astype(F32) - product


def ask(map_ref, owner, part_ref, out_ref):
    pivot_blocks = part_ref.shape[1] // BLOCK
    for j in range(out_ref.shape[1] // BLOCK):
        target = map_ref[0, owner, j]
        block = part_ref[:, at_block(lax.min(target, pivot_blocks - 1))]
        out_ref[:, static_block(j)] = jnp.where(
            target < pivot_blocks, block, jnp.zeros_like(block)
        )


def mid_back_kernel(members, late, map_ref, inverse_ref, border_ref, back_ref, *refs):
    values = refs[:-3]
    part_ref, asked_ref, piece_ref = refs[-3:]
    back = back_ref[...] - border_product(members, values, late, border_ref)
    part_ref[...] = times(back.astype(BF16), inverse_ref[0]).astype(BF16)
    owner = traced_partner(lax.axis_index(MEMBER), members - 1, members)
    ask(map_ref, owner, part_ref, asked_ref)
    piece_ref[...] = part_ref[:, at_part(owner, piece_ref.shape[1])]


def mid_share_kernel(members, step, map_ref, part_ref, asked_ref, piece_ref):
    owner = traced_partner(lax.axis_index(MEMBER), step, members)
    ask(map_ref, owner, part_ref, asked_ref)
    piece_ref[...] = part_ref[:, at_part(owner, piece_ref.shape[1])]


def pick_kernel(members, map_ref, part_ref, *refs):
    values = refs[:-2]
    base_ref, own_ref = refs[-2:]
    member = lax.axis_index(MEMBER)
    pivot_blocks = part_ref.shape[1] // BLOCK
    rows = values[0].shape[1]
    for j in range(base_ref.shape[1] // BLOCK):
        target = map_ref[0, member, j]

        @pl.when(target < pivot_blocks)
        def _():
            base_ref[:, static_block(j)] = part_ref[:, at_block(target)]

        border = target - pivot_blocks
        for k, values_ref in enumerate(values):
            owner = traced_source(member, k // 2, members)
            inner = border - (2 * owner + k % 2) * (rows // BLOCK)

            @pl.when((border >= 0) & (inner >= 0) & (inner < rows // BLOCK))
            def _():
                base_ref[:, static_block(j)] = values_ref[:, at_block(inner)]

    own_ref[...] = part_ref[:, at_part(member, own_ref.shape[1])]


def leaf_back_kernel(*refs):
    factor_ref, edge_ref, forward_ref = refs[:3]
    terms = refs[3:-1]
    out_ref = refs[-1]
    picked = terms[0][...].astype(F32)
    for term in terms[1:]:
        picked = picked + term[...].astype(F32)
    back = forward_ref[...].astype(F32) - times(picked.astype(BF16), edge_ref[...])
    back = back.astype(BF16)
    chunks = chunks_of(factor_ref.shape[0])
    for first, rows in chunks:
        total = None
        for lower, size in chunks:
            if lower >= first:
                factor = factor_ref[pl.ds(lower, size), pl.ds(first, rows)]
                part = times(back[:, lower : lower + size], factor)
                total = part if total is None else total + part
        out_ref[0, 0, pl.ds(first, rows), :] = total.astype(BF16).T


def mid_out_kernel(*refs):
    total = refs[0][...].astype(F32)
    for term in refs[1:-1]:
        total = total + term[...].astype(F32)
    refs[-1][0] = total.astype(BF16).T


def call(kernel, inputs, outs, scratch=(), flops=0, space=pltpu.VMEM):
    vmem = pl.BlockSpec(memory_space=pltpu.VMEM)
    smem = pl.BlockSpec(memory_space=pltpu.SMEM)
    in_specs = [smem if x.dtype == jnp.int32 else vmem for x in inputs]
    out_shape = [jax.ShapeDtypeStruct(shape, dtype) for shape, dtype in outs]
    if space == pltpu.HBM:
        in_specs = [pl.BlockSpec(memory_space=space)] * len(inputs)
        inputs = [pltpu.with_memory_space_constraint(x, space) for x in inputs]
        out_shape = [
            (pltpu.SMEM if dtype == jnp.int32 else pltpu.VMEM)(shape, dtype)
            for shape, dtype in outs
        ]
    moved = sum(x.size * x.dtype.itemsize for x in inputs)
    return pl.pallas_call(
        kernel,
        in_specs=in_specs,
        out_specs=[smem if dtype == jnp.int32 else vmem for _, dtype in outs],
        out_shape=out_shape,
        scratch_shapes=list(scratch),
        compiler_params=pltpu.CompilerParams(vmem_limit_bytes=VMEM_LIMIT),
        cost_estimate=pl.CostEstimate(flops=flops, bytes_accessed=moved, transcendentals=0),
    )(*inputs)


def total_of(first, others):
    total = first.astype(F32)
    for other in others:
        total = total + other.astype(F32)
    return total.astype(BF16)


def chips_of(groups, rows_out):
    chips = groups // 2
    return chips if is_split(chips) and rows_out % (2 * BLOCK) == 0 else 1


def group_sum(mine, other, size, chips):
    if not is_split(chips):
        total = total_of(mine[0], [exchange(other[0], GROUP, 1, size)])
        total = total_of(total, [exchange(total, GROUP, k, size) for k in range(2, size, 2)])
        return [total], [exchange(total, GROUP, 1, size)]
    own_units, other_units = [], []
    for kept, given in zip(mine, other):
        rows = kept.shape[1] // 2
        block = rows // 2
        low, high = split(kept, rows)
        low_core, high_core = split(exchange(given, GROUP, 1, size), rows)
        pair = exchange(total_of(high, [high_core]), GROUP, 2, size)
        side = total_of(low, [low_core, pair])
        far, near = split(exchange(side, GROUP, 4, size), block)
        unit = total_of(side, [jnp.concatenate([near, far], axis=1)])
        rest = exchange(unit, GROUP, 2, size)
        own_units += [unit, rest]
        other_units += [exchange(unit, GROUP, 1, size), exchange(rest, GROUP, 1, size)]
    return own_units, other_units


def member_sum(low, high, size):
    if not is_power_of_two(size):
        return lax.psum(low, MEMBER), lax.psum(high, MEMBER)
    steps = [1 << i for i in range(size.bit_length() - 1)]
    for first, second in zip(steps, reversed(steps)):
        other_low = exchange(low, MEMBER, first, size)
        other_high = exchange(high, MEMBER, second, size)
        low, high = total_of(low, [other_low]), total_of(high, [other_high])
    return low, high


def split(values, rows):
    return values[:, :rows], values[:, rows:]


def scatter_sum(pieces, size):
    rows = pieces[0][0].shape[1]
    if size != 4:
        arrived = [
            split(exchange(jnp.concatenate(pair, axis=1), MEMBER, k, size), rows)
            for k, pair in enumerate(pieces, start=1)
        ]
        return [low for low, _ in arrived], [high for _, high in arrived]
    (low1, high1), (low2, high2), (low3, high3) = pieces
    relay1 = exchange(low3, MEMBER, 1, size)
    relay2 = exchange(high3, MEMBER, 2, size)
    first1 = exchange(low1, MEMBER, 1, size)
    first2 = exchange(high2, MEMBER, 2, size)
    last2 = exchange(total_of(low2, [relay1]), MEMBER, 2, size)
    last1 = exchange(total_of(high1, [relay2]), MEMBER, 1, size)
    return [first1, last2], [first2, last1]


def gather(low, high, size):
    rows = low.shape[1]
    if size != 4:
        values = jnp.concatenate([low, high], axis=1)
        return [(low, high)] + [
            split(exchange(values, MEMBER, k, size), rows) for k in range(1, size)
        ]
    high1 = exchange(high, MEMBER, 1, size)
    low2 = exchange(low, MEMBER, 2, size)
    low1 = exchange(low, MEMBER, 1, size)
    high2 = exchange(high, MEMBER, 2, size)
    low3 = exchange(low2, MEMBER, 1, size)
    high3 = exchange(high1, MEMBER, 2, size)
    return [(low, high), (low1, high1), (low2, high2), (low3, high3)]


def make_on_device(groups, members):
    steps = range(1, members)

    def on_device(
        rhs,
        leaf_pivot_inverse,
        leaf_border_block,
        leaf_map,
        mid_inverse,
        mid_border,
        root_map,
        root_inverse,
    ):
        columns = rhs.shape[3]
        leaf_pivots = rhs.shape[2]
        leaf_rows = leaf_border_block.shape[2]
        own_pivots, pivots = mid_inverse.shape[1:]
        border_rows = mid_border.shape[1]
        own_border = border_rows // members
        row_count, share_rows = root_inverse.shape
        half = share_rows // 2
        rows_out = share_rows // groups

        def flat(rows, dtype=BF16):
            return ((columns, rows), dtype)

        def spread_over_members(values):
            return [values] + [exchange(values, MEMBER, k, members) for k in steps]

        leaf_forward, leaf_factor, leaf_edge, leaf_map, root_map = call(
            leaf_forward_kernel,
            [rhs, leaf_pivot_inverse, leaf_border_block, leaf_map, root_map],
            [
                flat(leaf_pivots),
                (leaf_pivot_inverse.shape[2:], BF16),
                (leaf_border_block.shape[2:], BF16),
                (leaf_map.shape, jnp.int32),
                (root_map.shape, jnp.int32),
            ],
            [
                pltpu.VMEM((leaf_pivots, columns), BF16),
                pltpu.SemaphoreType.DMA((4 + len(chunks_of(leaf_pivots)),)),
            ],
            flops=2 * columns * leaf_pivots * leaf_pivots,
            space=pltpu.HBM,
        )
        (leaf_out,) = call(
            leaf_out_kernel, [leaf_forward, leaf_edge], [flat(leaf_rows)], flops=PREFETCH_FLOPS
        )
        terms = spread_over_members(leaf_out)
        mid_forward = []
        groups_of_terms = [[0], list(steps)]
        if members == 4:
            groups_of_terms = [[0], [3], [2, 1]]
        for which in groups_of_terms:
            last = which is groups_of_terms[-1]
            mid_forward = call(
                functools.partial(mid_forward_kernel, members, which),
                [leaf_map, mid_inverse, *(terms[k] for k in which), *mid_forward],
                [flat(own_pivots, BF16 if last else F32)],
                flops=2 * columns * own_pivots * leaf_rows * len(which),
            )
        (mid_forward,) = mid_forward
        half_border = own_border // 2
        pieces = {k: () for k in steps}
        for k in reversed(steps):
            for halves in [(0,), (1,)] if k == members - 1 else [(0, 1)]:
                pieces[k] += tuple(
                    call(
                        functools.partial(mid_piece_kernel, members, k, halves),
                        [mid_border, mid_forward],
                        [flat(half_border)] * len(halves),
                        flops=columns * own_pivots * own_border * len(halves),
                    )
                )
        lows, highs = scatter_sum([pieces[k] for k in steps], members)
        (own_update,) = call(
            functools.partial(own_update_kernel, members, pivots // BLOCK),
            [leaf_map, mid_border, mid_forward, *terms],
            [flat(own_border, F32)],
            flops=2 * columns * own_pivots * own_border,
        )
        chips = chips_of(groups, rows_out)
        whole_share = pltpu.VMEM((columns, share_rows), BF16)
        half_streams = [flat(half // 2)] * 2 if is_split(chips) else [flat(half)]
        count = len(half_streams)
        streams = call(
            functools.partial(root_term_kernel, chips, len(lows)),
            [root_map, own_update, *lows, *highs],
            half_streams * 2,
            [whole_share],
        )
        units = group_sum(streams[count:], streams[:count], groups, chips)
        if is_split(chips):
            waves = [
                [(1, 0), (1, 2)],
                [(0, 0), (0, 2), (1, 1)],
                [(1, 3), (0, 1)],
                [(0, 3)],
            ]
        else:
            waves = [[(1, 0)], [(0, 0)]]
        root_flops = columns * row_count * share_rows
        half_count = row_count // 2
        before = []
        for which in waves[:-1]:
            before = call(
                functools.partial(root_early_kernel, chips, which),
                [root_inverse, *(units[1 - own][k] for own, k in which), *before],
                [flat(half_count, F32), flat(half_count, F32)],
                flops=root_flops // 2,
            )
        root_parts = [
            call(
                functools.partial(root_forward_kernel, chips, waves[-1], part),
                [root_inverse, *(units[1 - own][k] for own, k in waves[-1]), total],
                [flat(half_count)],
                flops=root_flops // 4,
            )[0]
            for part, total in enumerate(before)
        ]
        root_forward = member_sum(*root_parts, members)
        streams = [(own, number) for own in (0, 1) for number in range(count)]
        first = call(
            functools.partial(root_back_kernel, chips, streams, 0),
            [root_inverse, root_forward[0]],
            [(shape, F32) for shape, _ in half_streams * 2],
            flops=root_flops,
        )
        halves = []
        for begin, end in [(i, i + 1) for i in range(count)] + [(count, 2 * count)]:
            halves += call(
                functools.partial(root_back_kernel, chips, streams[begin:end], 1),
                [root_inverse, root_forward[1], *first[begin:end]],
                half_streams[: end - begin],
                flops=root_flops * (end - begin) // (2 * count),
            )
        other, mine = halves[:count], halves[count:]
        mine, other = group_sum(mine, other, groups, chips)
        own_values = call(
            functools.partial(root_pick_kernel, chips),
            [root_map, *mine, *other],
            [flat(half_border), flat(half_border)],
            [whole_share],
        )
        shape = [((1, rows_out, columns), BF16)]
        if is_split(chips):
            (root_out,) = call(root_out_kernel, [mine[0], mine[2]], shape)
        else:
            turned = pltpu.VMEM((max(rows_out, BLOCK), columns), F32)
            (root_out,) = call(root_slice_kernel, [*mine, *other], shape, [whole_share, turned])
        values = gather(*own_values, members)
        if members == 4:
            waves = [[(0, 0), (0, 1), (1, 1), (2, 0)], [(1, 0), (2, 1)], [(3, 0), (3, 1)]]
        else:
            waves = [[(0, 0), (0, 1)], [(k, h) for k in steps for h in range(2)]]
        back = mid_forward
        for which in waves[:-1]:
            (back,) = call(
                functools.partial(mid_early_kernel, members, which),
                [mid_border, back] + [values[k][h] for k, h in which],
                [flat(own_pivots, F32)],
                flops=2 * columns * own_pivots * half_border * len(which),
            )
        part, *last_pair = call(
            functools.partial(mid_back_kernel, members, waves[-1]),
            [leaf_map, mid_inverse, mid_border, back] + [values[k][h] for k, h in waves[-1]],
            [flat(pivots), flat(leaf_rows), flat(own_pivots)],
            flops=2 * columns * own_pivots * (pivots + half_border * len(waves[-1])),
        )
        pairs = [
            call(
                functools.partial(mid_share_kernel, members, k),
                [leaf_map, part],
                [flat(leaf_rows), flat(own_pivots)],
                flops=SHARE_FLOPS,
            )
            for k in steps[:-1]
        ]
        picked, pieces = scatter_sum([*pairs, last_pair], members)
        base, own_piece = call(
            functools.partial(pick_kernel, members),
            [leaf_map, part] + [half for pair in values for half in pair],
            [flat(leaf_rows), flat(own_pivots)],
            flops=SHARE_FLOPS,
        )
        (leaf_values,) = call(
            leaf_back_kernel,
            [leaf_factor, leaf_edge, leaf_forward, base, *picked],
            [((1, 1, leaf_pivots, columns), BF16)],
            flops=2 * columns * leaf_pivots * (leaf_pivots + leaf_rows),
        )
        (mid_out,) = call(mid_out_kernel, [own_piece, *pieces], [((1, own_pivots, columns), BF16)])
        return leaf_values, mid_out, root_out

    return on_device


def solution(mesh):
    in_specs = (
        P(GROUP, MEMBER, None, None),
        P(GROUP, MEMBER, None, None),
        P(GROUP, MEMBER, None, None),
        P(GROUP, None, None),
        P(GROUP, MEMBER, None),
        P(GROUP, None, MEMBER),
        P(GROUP, MEMBER, None),
        P(GROUP, MEMBER),
    )
    out_specs = (
        P(GROUP, MEMBER, None, None),
        P(GROUP, MEMBER, None),
        P(MEMBER, GROUP, None),
    )
    on_device = make_on_device(mesh.shape[GROUP], mesh.shape[MEMBER])

    return jax.shard_map(
        on_device, mesh=mesh, in_specs=in_specs, out_specs=out_specs, check_vma=False
    )
```
